256 devices in a mesh: grp: 8 (over z_hi, x), slab: 32 (over z_lo, y, core).
Axes of the slice: x: 4, y: 4, z: 8 (z_hi: 2, z_lo: 4; z = z_hi * 4 + z_lo), core: 2. Of those that a mesh axis runs over, the one named last changes fastest.
Arguments:
- sample_xy: float32 [8, 32, 8, 2, 256], P('grp', 'slab'), may hold values from 0 to 384
- sample_dz: float32 [8, 32, 8, 256], P('grp', 'slab'), may hold values from 0 to 1
- sample_values: float32 [8, 32, 8, 2, 256], P('grp', 'slab'), may hold values from -6 to 6
- block_tile: int32 [8, 32, 8], P('grp', 'slab'), may hold values from 0 to 5
- block_count: int32 [8, 32, 8], P('grp', 'slab'), may hold values from 1 to 256
Outputs:
- grid_sum: float32 [384, 192, 2, 384], P('grp', 'slab')
The draws below stay inside these ranges and needn't reach their ends.
Inputs may be any that keep to these rules, and one draw needn't show every extreme that they name: `block_tile`: the base plane of every sample of a block. Slots from block_count on hold values that are not used.
All inputs are finite; a program needn't handle non-finite values.
Results may differ from the reference program's by a relative error of at most 0.0037.
Values sent between devices are 32-bit elements; how exact they have to be, the bound alone decides.
A program may use at most 192 MiB of HBM per device.

```python
import math
import jax
import jax.numpy as jnp
from jax import lax

NX = 384
NY = 384
BLOCK = 256
PLANES = 6
BLOCKS_DEV = 8
NZ = 192
N_GRP = 8
N_SLAB = 32


def place_ends(array, rng, smallest, high):
    shape = array.shape
    index_at = [jax.random.randint(jax.random.fold_in(rng, axis), (), 0, shape[axis]) for axis in range(len(shape))]
    array = array.at[tuple(index_at)].set(smallest)
    longest = shape.index(max(shape))
    index_at[longest] = (index_at[longest] + 1) % shape[longest]
    return array.at[tuple(index_at)].set(high)


def block_scale(key, dims, pieces, smallest, high):
    loudness, own = 1.0, jax.random.fold_in(key, 6)
    for axis_at, parts in pieces:
        draws = jnp.exp(jax.random.uniform(jax.random.fold_in(own, axis_at), (parts,), jnp.float32, smallest / len(pieces), high / len(pieces)))
        loudness = loudness * jnp.repeat(draws, dims[axis_at] // parts).reshape([-1 if axis == axis_at else 1 for axis in range(len(dims))])
    return loudness


def centred(own_key, shape, scale, most, shards=(), kind=jnp.bfloat16):
    array = jax.random.normal(own_key, shape, jnp.float32) * scale
    if len(shards) > 0:
        array = block_scale(own_key, shape, shards, -0.22, 0.18) * array
    return jnp.clip(array, min=-most, max=most).astype(kind)


def setup_inputs(seed: int = 0) -> dict:
    arg_keys = jax.random.split(jax.random.key(seed), 6)
    sample_xy = jnp.clip(384.0 * jax.random.uniform(arg_keys[0], (N_GRP, N_SLAB, BLOCKS_DEV, 2, BLOCK), jnp.float32) ** block_scale(arg_keys[0], (N_GRP, N_SLAB, BLOCKS_DEV, 2, BLOCK), ((0, 8), (1, 32)), -0.2, 0.2), 0.0, 384.0)
    sample_dz = jnp.clip(1.0 * jax.random.uniform(arg_keys[1], (N_GRP, N_SLAB, BLOCKS_DEV, BLOCK), jnp.float32) ** block_scale(arg_keys[1], (N_GRP, N_SLAB, BLOCKS_DEV, BLOCK), ((0, 8), (1, 32)), -0.2, 0.2), 0.0, 1.0)
    sample_values = centred(arg_keys[2], (N_GRP, N_SLAB, BLOCKS_DEV, 2, BLOCK), 1.0, 6.0, ((0, 8), (1, 32)), jnp.float32)
    block_tile = place_ends(jax.random.randint(arg_keys[3], (N_GRP, N_SLAB, BLOCKS_DEV), 0, PLANES), jax.random.fold_in(arg_keys[3], 1), 0, PLANES - 1).astype(jnp.int32)
    block_count = place_ends(jax.random.randint(arg_keys[4], (N_GRP, N_SLAB, BLOCKS_DEV), 1, BLOCK + 1), jax.random.fold_in(arg_keys[4], 1), 1, BLOCK).astype(jnp.int32)
    return dict(sample_xy=sample_xy, sample_dz=sample_dz, sample_values=sample_values, block_tile=block_tile, block_count=block_count)


BETA = math.pi * math.sqrt(19.45)

def kaiser_top():
    half_sq = (0.5 * BETA) ** 2
    term = 1.0
    total = 1.0
    for order in range(1, 32):
        term = term * half_sq / (order * order)
        total = total + term
    return total - 1.0

def bessel_zero(arg):
    half_sq = 0.5 * arg * (0.5 * arg)
    term = jnp.ones_like(arg)
    total = term
    for order in range(1, 32):
        term = term * half_sq / float(order * order)
        total = total + term
    return total

def kaiser(distance):
    inside = jnp.maximum(1.0 - (distance / 3.0) ** 2, 0.0)
    bessel = bessel_zero(BETA * jnp.sqrt(inside))
    return (bessel - 1.0) / kaiser_top()

def reference(sample_xy, sample_dz, sample_values, block_tile, block_count):
    offsets = jnp.arange(6).astype(sample_xy.dtype)
    offsets_int = jnp.arange(6).astype(jnp.int32)
    lane_ids = jnp.arange(BLOCK).astype(jnp.int32)
    index_c = jnp.arange(2).astype(jnp.int32)

    def one_slab(slab_id, grid_sum):
        coords = lax.dynamic_index_in_dim(sample_xy, slab_id, 1, keepdims=False).reshape(-1, 2, BLOCK)
        depths = lax.dynamic_index_in_dim(sample_dz, slab_id, 1, keepdims=False).reshape(-1, BLOCK)
        values = lax.dynamic_index_in_dim(sample_values, slab_id, 1, keepdims=False).reshape(-1, 2, BLOCK)
        tile_ids = lax.dynamic_index_in_dim(block_tile, slab_id, 1, keepdims=False).reshape(-1)
        counts = lax.dynamic_index_in_dim(block_count, slab_id, 1, keepdims=False).reshape(-1)
        pos_x = coords[:, 0]
        pos_y = coords[:, 1]
        cell_x = jnp.floor(pos_x)[..., None] - 2.0 + offsets
        cell_y = jnp.floor(pos_y)[..., None] - 2.0 + offsets
        weight_x = lax.optimization_barrier(kaiser(cell_x - pos_x[..., None]).astype(jnp.bfloat16)).astype(jnp.float32)
        weight_y = kaiser(cell_y - pos_y[..., None])
        weight_z = kaiser(offsets - 2.0 - depths[..., None])
        keep_mask = (lane_ids[None, :] < counts[:, None]).astype(jnp.float32)
        spread_w = (weight_z * keep_mask[..., None])[:, :, :, None, None] * jnp.swapaxes(values, 1, 2)[:, :, None, :, None] * weight_y[:, :, None, None, :]
        spread_w = lax.optimization_barrier(spread_w.astype(jnp.bfloat16)).astype(jnp.float32)
        contrib = weight_x[:, :, :, None, None, None] * spread_w[:, :, None]
        index_x = jnp.mod(cell_x.astype(jnp.int32), NX)
        index_y = jnp.mod(cell_y.astype(jnp.int32), NY)
        index_z = jnp.mod(slab_id * PLANES + tile_ids[:, None] + offsets_int[None, :] - 2, NZ)
        return grid_sum.at[index_x[:, :, :, None, None, None], index_z[:, None, None, :, None, None], index_c[None, None, None, None, :, None], index_y[:, :, None, None, None, :]].add(contrib)
    start_grid = jnp.zeros((NX, NZ, 2, NY), jnp.float32)
    return lax.fori_loop(0, N_SLAB, one_slab, start_grid)
```

```python
import math

import jax
import jax.numpy as jnp
from jax import lax
from jax.experimental import pallas as pl
from jax.experimental.pallas import tpu as pltpu
from jax.sharding import PartitionSpec as P

NX = 384
NY = 384
PLANES = 6
BLOCKS = 8
GROUPS = 8
ROWS = 48
FIELDS = 6
HALF_ROWS = FIELDS * BLOCKS
SEND_ROWS = 2 * HALF_ROWS
MESH = pl.DeviceIdType.MESH
BETA = math.pi * math.sqrt(19.45)
F32 = jnp.float32
BF16 = jnp.bfloat16
I32 = jnp.int32


def kaiser_coefficients():
    half_sq = (0.5 * BETA) ** 2
    terms = []
    term = 1.0
    for order in range(1, 32):
        term = term * half_sq / (order * order)
        terms.append(term)
    top = sum(terms)
    return [value / top for value in terms]


COEFF = kaiser_coefficients()


def kaiser(distance):
    third = distance * (1.0 / 3.0)
    inside = jnp.maximum(1.0 - third * third, 0.0)
    square = inside * inside
    fourth = square * square
    chains = []
    for first in range(4):
        picked = COEFF[first::4]
        total = jnp.full_like(inside, picked[-1])
        for value in picked[-2::-1]:
            total = total * fourth + value
        chains.append(total)
    low = chains[0] + chains[1] * inside
    high = chains[2] + chains[3] * inside
    return (low + high * square) * inside


def sort_kernel(tile_ref, count_ref, xy_ref, dz_ref, val_ref, out_ref, fields):
    lanes = lax.broadcasted_iota(I32, (BLOCKS, 256), 1)
    subs = lax.broadcasted_iota(I32, (BLOCKS, 256), 0)
    counts = jnp.zeros((BLOCKS, 256), I32)
    tiles = jnp.zeros((BLOCKS, 256), I32)
    for b in range(BLOCKS):
        counts = jnp.where(subs == b, count_ref[0, 0, b], counts)
        tiles = jnp.where(subs == b, tile_ref[0, 0, b], tiles)
    along_x = xy_ref[:, 0, :]
    cell = jnp.floor(along_x)
    shifted = cell + 3.0
    shifted = jnp.where(shifted >= NX, shifted - NX, shifted)
    shifted = jnp.where(lanes < counts, shifted, 400.0)
    fields[0:8] = along_x
    fields[8:16] = xy_ref[:, 1, :]
    fields[16:24] = dz_ref[...]
    fields[24:32] = val_ref[:, 0, :]
    fields[32:40] = val_ref[:, 1, :]
    table = jnp.where(lanes == 17, tiles.astype(F32), 0.0)
    for at in range(17):
        if at < 8:
            bound = float(ROWS * at)
        elif at < 16:
            bound = float(ROWS * (at - 8) + ROWS + 5)
        else:
            bound = 5.0
        below = jnp.sum(jnp.where(shifted < bound, 1.0, 0.0), axis=1, keepdims=True)
        table = jnp.where(lanes == at, below, table)
    key = shifted * 256.0 + lanes.astype(F32)
    key_t = key.T
    place = lax.broadcasted_iota(I32, (256, 256), 0).astype(F32)
    for b in range(BLOCKS):
        before = key_t[:, b : b + 1] < key[b : b + 1, :]
        rank = jnp.sum(jnp.where(before, 1.0, 0.0), axis=0, keepdims=True)
        pick = jnp.where(place == rank, 1.0, 0.0).astype(BF16)
        rows = jnp.concatenate([fields[f * 8 + b : f * 8 + b + 1, :] for f in range(5)] + [jnp.zeros((3, 256), F32)], axis=0)
        top = rows.astype(BF16)
        rest = rows - top.astype(F32)
        mid = rest.astype(BF16)
        low = (rest - mid.astype(F32)).astype(BF16)
        parts = jnp.concatenate([top.astype(F32), mid.astype(F32), low.astype(F32)], axis=0).astype(BF16)
        moved = lax.dot_general(parts, pick, (((1,), (1,)), ((), ())), preferred_element_type=F32)
        ordered = (moved[0:8] + moved[8:16]) + moved[16:24]
        for f in range(5):
            for half in range(2):
                out_ref[half * HALF_ROWS + f * 8 + b : half * HALF_ROWS + f * 8 + b + 1, :] = ordered[
                    f : f + 1, half * 128 : half * 128 + 128
                ]
    out_ref[40:48, :] = table[:, 0:128]
    out_ref[HALF_ROWS + 40 : HALF_ROWS + 48, :] = table[:, 128:256]


def sort_blocks(tile, count, xy, dz, val):
    smem = pl.BlockSpec(memory_space=pltpu.SMEM)
    vmem = pl.BlockSpec(memory_space=pltpu.VMEM)
    return pl.pallas_call(
        sort_kernel,
        out_shape=jax.ShapeDtypeStruct((SEND_ROWS, 128), F32),
        in_specs=[smem, smem, vmem, vmem, vmem],
        out_specs=vmem,
        scratch_shapes=[pltpu.VMEM((40, 256), F32)],
        name="sort_blocks",
    )(tile, count, xy, dz, val)


def exchange_kernel(own_ref, out_ref, send_sem, recv_sem, copy_sem):
    grp = lax.axis_index("grp")
    slab = lax.axis_index("slab")
    far = lax.rem(grp + 4, 8)
    half = (grp // 4) * 4
    spot = grp - half
    peers = [half + lax.rem(spot + step, 4) for step in (1, 3, 2)]
    far_half = 4 - half
    up = lax.rem(slab + 1, 32)
    down = lax.rem(slab + 31, 32)
    around = [(far, slab)] + [(peer, slab) for peer in peers] + [(grp, up), (grp, down)]

    barrier = pltpu.get_barrier_semaphore()
    for device in around:
        pl.semaphore_signal(barrier, inc=1, device_id=device, device_id_type=MESH)

    own_copy = pltpu.make_async_copy(own_ref, out_ref.at[0, grp], copy_sem)
    own_copy.start()
    pl.semaphore_wait(barrier, len(around))

    sends = []

    def send(source, kind, owner, sem, device):
        copy = pltpu.make_async_remote_copy(
            src_ref=source,
            dst_ref=out_ref.at[kind, owner],
            send_sem=send_sem.at[len(sends)],
            recv_sem=recv_sem.at[sem],
            device_id=device,
            device_id_type=MESH,
        )
        copy.start()
        sends.append(copy)
        return copy

    def arrive(kind, owner, sem):
        pltpu.make_async_remote_copy(
            src_ref=own_ref,
            dst_ref=out_ref.at[kind, owner],
            send_sem=send_sem.at[0],
            recv_sem=recv_sem.at[sem],
            device_id=(grp, slab),
            device_id_type=MESH,
        ).wait_recv()

    send(own_ref, 0, grp, 0, (far, slab))
    for at, peer in enumerate(peers):
        send(own_ref, 0, grp, 1 + at, (peer, slab))
    send(own_ref, 1, grp, 7, (grp, up))
    send(own_ref, 2, grp, 15, (grp, down))
    back = [half + lax.rem(spot + step, 4) for step in (3, 1, 2)]
    for at in range(3):
        arrive(0, back[at], 1 + at)
        send(out_ref.at[0, back[at]], 1, back[at], 8 + at, (grp, up))
        send(out_ref.at[0, back[at]], 2, back[at], 16 + at, (grp, down))
    arrive(0, far, 0)
    for at, peer in enumerate(peers):
        send(out_ref.at[0, far], 0, far, 4 + at, (peer, slab))
    send(out_ref.at[0, far], 1, far, 11, (grp, up))
    send(out_ref.at[0, far], 2, far, 19, (grp, down))
    for at in range(3):
        owner = back[at] - half + far_half
        arrive(0, owner, 4 + at)
        send(out_ref.at[0, owner], 1, owner, 12 + at, (grp, up))
        send(out_ref.at[0, owner], 2, owner, 20 + at, (grp, down))
    for kind, base in ((1, 7), (2, 15)):
        arrive(kind, grp, base)
        arrive(kind, far, base + 4)
        for at in range(3):
            arrive(kind, back[at], base + 1 + at)
            arrive(kind, back[at] - half + far_half, base + 5 + at)
    own_copy.wait()
    for copy in sends:
        copy.wait_send()


def exchange(own):
    vmem = pl.BlockSpec(memory_space=pltpu.VMEM)
    return pl.pallas_call(
        exchange_kernel,
        out_shape=jax.ShapeDtypeStruct((3, GROUPS, SEND_ROWS, 128), F32),
        in_specs=[pl.BlockSpec(memory_space=pl.ANY)],
        out_specs=vmem,
        scratch_shapes=[pltpu.SemaphoreType.DMA((23,)), pltpu.SemaphoreType.DMA((23,)), pltpu.SemaphoreType.DMA],
        compiler_params=pltpu.CompilerParams(collective_id=0, has_side_effects=True),
        name="exchange",
    )(own)


def grid_kernel(read_group, all_ref, out_ref, table_v, table, packed, lhs, rhs, total, sem):
    group = read_group()
    sources = 3 * GROUPS
    for source in range(sources):
        table_v[source * 8 : source * 8 + 8, :] = all_ref[source * SEND_ROWS + 40 : source * SEND_ROWS + 48, :].astype(I32)
    copy = pltpu.make_async_copy(table_v, table, sem)
    copy.start()
    total[...] = jnp.zeros_like(total)
    lanes = lax.broadcasted_iota(I32, (8, 128), 1)
    subs = lax.broadcasted_iota(I32, (8, 128), 0)
    copy.wait()

    def depth_shift(kind, tile):
        return tile + (0, -PLANES, PLANES)[kind]

    def wanted(kind, tile):
        return (True, tile >= 3, tile <= 1)[kind]

    def append(kind, source, b, half, low, count, offset):
        tile = table[source * 8 + b, 17]
        values = all_ref[pl.ds(source * SEND_ROWS + half * HALF_ROWS + b, FIELDS, stride=8), :]
        values = jnp.where(subs[:FIELDS] == 2, values + depth_shift(kind, tile).astype(F32), values)
        at = lax.bitwise_and(offset, 127)
        rolled = pltpu.roll(values, lax.bitwise_and(at - low + 128, 127), 1)
        slot = lax.shift_right_logical(offset, 7)
        packed[slot, 0:FIELDS] = jnp.where(lanes[:FIELDS] >= at, rolled, packed[slot, 0:FIELDS])
        packed[slot + 1, 0:FIELDS] = rolled
        return offset + count

    def window(kind, source, b):
        row = source * 8 + b
        start = table[row, group]
        count = table[row, 8 + group] - start
        if kind > 0:
            count = jnp.where(wanted(kind, table[row, 17]), count, 0)
        half = jnp.minimum(lax.shift_right_logical(start, 7), 1)
        low = lax.bitwise_and(start, 127)
        first = jnp.minimum(count, 128 - low)
        return half, low, first, count - first

    def gather_first(kind):
        def body(at, carry):
            offset, more = carry
            source = kind * GROUPS + at
            for b in range(BLOCKS):
                half, low, first, left = window(kind, source, b)
                offset = append(kind, source, b, half, low, first, offset)
                more = more + left
            return offset, more

        return body

    offset = jnp.int32(0)
    for kind in range(3):
        offset, more = lax.fori_loop(0, GROUPS, gather_first(kind), (offset, jnp.int32(0)))

        def gather_rest(at, offset):
            source = kind * GROUPS + lax.shift_right_logical(at, 3)
            b = lax.bitwise_and(at, 7)
            left = window(kind, source, b)[3]
            return lax.cond(left > 0, lambda o: append(kind, source, b, 1, 0, left, o), lambda o: o, offset)

        offset = lax.fori_loop(0, jnp.where(more > 0, 64, 0), gather_rest, offset)

        def gather_wrap(at, offset):
            source = kind * GROUPS + lax.shift_right_logical(at, 3)
            b = lax.bitwise_and(at, 7)
            row = source * 8 + b
            count = table[row, 16]
            if kind > 0:
                count = jnp.where(wanted(kind, table[row, 17]), count, 0)

            def add(o):
                o = append(kind, source, b, 0, 0, jnp.minimum(count, 128), o)
                left = count - jnp.minimum(count, 128)
                return lax.cond(left > 0, lambda p: append(kind, source, b, 1, 0, left, p), lambda p: p, o)

            return lax.cond(count > 0, add, lambda o: o, offset)

        offset = lax.fori_loop(0, jnp.where(group == GROUPS - 1, 64, 0), gather_wrap, offset)

    subs_f = subs.astype(F32)
    first_row = (group * ROWS).astype(F32)

    def pick(weights, index):
        return jnp.take_along_axis(weights, index, axis=0, mode="promise_in_bounds")

    def chunk(at, carry):
        for half in range(2):
            cols = slice(half * 128, half * 128 + 128)
            values = packed[at * 2 + half]
            values = jnp.where(lanes + (at * 256 + half * 128) < offset, values, 0.0)
            along_x, along_y, along_z = [jnp.broadcast_to(values[f : f + 1], (8, 128)) for f in range(3)]
            cell_x = jnp.floor(along_x)
            cell_y = jnp.floor(along_y)
            taps_x = kaiser(subs_f - 2.0 - (along_x - cell_x))
            taps_y = kaiser(subs_f - 2.0 - (along_y - cell_y))
            taps_z = kaiser(subs_f - along_z)
            base_x = cell_x - 2.0 - first_row
            base_x = jnp.where(base_x < -192.0, base_x + NX, base_x)
            base_x = jnp.where(base_x >= 192.0, base_x - NX, base_x)
            base_y = cell_y - 2.0
            base_y = jnp.where(base_y < 0.0, base_y + NY, base_y)
            base_y = jnp.where(base_y >= NY, base_y - NY, base_y)
            away_x = subs - base_x.astype(I32)
            away_y = subs - base_y.astype(I32)

            def spread(taps, away, rows, wrap):
                index = away + rows
                if wrap:
                    index = jnp.where(index < 0, index + NY, index)
                else:
                    index = jnp.where(index < 0, 7, index)
                return pick(taps, jnp.minimum(index, 7))

            for row in range(0, NY, 16):
                pair = [spread(taps_y, away_y, row + part, row + part == 0) for part in (0, 8)]
                rhs[row : row + 16, cols] = jnp.concatenate(pair, axis=0).astype(BF16)
            weights_x = [spread(taps_x, away_x, row, False).astype(BF16).astype(F32) for row in range(0, ROWS, 8)]
            for z in range(PLANES):
                for c in range(2):
                    scale = jnp.broadcast_to(taps_z[z : z + 1] * values[3 + c : 4 + c], (8, 128))
                    for row in range(0, ROWS, 16):
                        pair = [weights_x[(row + part) // 8] * scale for part in (0, 8)]
                        first = (z * 2 + c) * ROWS + row
                        lhs[first : first + 16, cols] = jnp.concatenate(pair, axis=0).astype(BF16)
        total[...] += lax.dot_general(lhs[...], rhs[...], (((1,), (1,)), ((), ())), preferred_element_type=F32)
        return carry

    lax.fori_loop(0, lax.shift_right_logical(offset + 255, 8), chunk, 0)
    for z in range(PLANES):
        for c in range(2):
            for y in range(3):
                first = (z * 2 + c) * ROWS
                out_ref[pl.ds(z * 6 + y * 2 + c, ROWS, stride=36), :] = total[first : first + ROWS, y * 128 : y * 128 + 128]


def grid_block(everything, group=None):
    vmem = pl.BlockSpec(memory_space=pltpu.VMEM)
    if group is None:
        operands, specs = [everything], [vmem]

        def kernel(all_ref, *refs):
            grid_kernel(lambda: lax.axis_index("grp"), all_ref, *refs)
    else:
        operands, specs = [group, everything], [pl.BlockSpec(memory_space=pltpu.SMEM), vmem]

        def kernel(group_ref, all_ref, *refs):
            grid_kernel(lambda: group_ref[0], all_ref, *refs)

    return pl.pallas_call(
        kernel,
        out_shape=jax.ShapeDtypeStruct((ROWS * PLANES * 6, 128), F32),
        in_specs=specs,
        out_specs=vmem,
        scratch_shapes=[
            pltpu.VMEM((192, 128), I32),
            pltpu.SMEM((192, 128), I32),
            pltpu.VMEM((388, 8, 128), F32),
            pltpu.VMEM((12 * ROWS, 256), BF16),
            pltpu.VMEM((NY, 256), BF16),
            pltpu.VMEM((12 * ROWS, NY), F32),
            pltpu.SemaphoreType.DMA,
        ],
        name="grid_block",
    )(*operands)


def finish(flat):
    return flat.reshape(ROWS, PLANES, 3, 2, 128).transpose(0, 1, 3, 2, 4).reshape(ROWS, PLANES, 2, NY)


def shards(sample_xy, sample_dz, sample_values, block_tile, block_count):
    own = sort_blocks(
        block_tile, block_count, sample_xy.reshape(8, 2, 256), sample_dz.reshape(8, 256), sample_values.reshape(8, 2, 256)
    )
    everything = exchange(own)
    return finish(grid_block(everything.reshape(3 * GROUPS * SEND_ROWS, 128)))


def solution(mesh):
    return jax.shard_map(
        shards,
        mesh=mesh,
        in_specs=(
            P("grp", "slab", None, None, None),
            P("grp", "slab", None, None),
            P("grp", "slab", None, None, None),
            P("grp", "slab", None),
            P("grp", "slab", None),
        ),
        out_specs=P("grp", "slab", None, None),
        check_vma=False,
    )
```

```python
import math

import jax
import jax.numpy as jnp
from jax import lax
from jax.experimental import pallas as pl
from jax.experimental.pallas import tpu as pltpu
from jax.sharding import PartitionSpec as P

NX = 384
NY = 384
PLANES = 6
BLOCKS = 8
GROUPS = 8
ROWS = 48
FIELDS = 5
HALF_ROWS = FIELDS * BLOCKS
TABLE = 2 * HALF_ROWS
SEND_ROWS = TABLE + BLOCKS
SOURCES = 3 * GROUPS
START, COUNT, WRAP = 0, 8, 32
MESH = pl.DeviceIdType.MESH
BETA = math.pi * math.sqrt(19.45)
F32 = jnp.float32
BF16 = jnp.bfloat16
I32 = jnp.int32


def kaiser_coefficients():
    half_sq = (0.5 * BETA) ** 2
    terms = []
    term = 1.0
    for order in range(1, 32):
        term = term * half_sq / (order * order)
        terms.append(term)
    top = sum(terms)
    return [value / top for value in terms]


COEFF = kaiser_coefficients()


def kaiser(distance):
    third = distance * (1.0 / 3.0)
    inside = jnp.maximum(1.0 - third * third, 0.0)
    square = inside * inside
    fourth = square * square
    chains = []
    for first in range(4):
        picked = COEFF[first::4]
        total = jnp.full_like(inside, picked[-1])
        for value in picked[-2::-1]:
            total = total * fourth + value
        chains.append(total)
    low = chains[0] + chains[1] * inside
    high = chains[2] + chains[3] * inside
    return (low + high * square) * inside


def sort_blocks(tile_ref, count_ref, xy_ref, dz_ref, val_ref, out_ref, fields):
    lanes = lax.broadcasted_iota(I32, (BLOCKS, 256), 1)
    subs = lax.broadcasted_iota(I32, (BLOCKS, 256), 0)
    counts = jnp.zeros((BLOCKS, 256), I32)
    tiles = jnp.zeros((BLOCKS, 256), I32)
    for b in range(BLOCKS):
        counts = jnp.where(subs == b, count_ref[0, 0, b], counts)
        tiles = jnp.where(subs == b, tile_ref[0, 0, b], tiles)
    along_x = xy_ref[:, 0, :]
    cell = jnp.floor(along_x)
    shifted = cell + 3.0
    shifted = jnp.where(shifted >= NX, shifted - NX, shifted)
    shifted = jnp.where(lanes < counts, shifted, 400.0)
    fields[0:8] = along_x
    fields[8:16] = xy_ref[:, 1, :]
    fields[16:24] = dz_ref[...] + tiles.astype(F32)
    fields[24:32] = val_ref[:, 0, :]
    fields[32:40] = val_ref[:, 1, :]

    def below(bound):
        return jnp.sum(jnp.where(shifted < bound, 1.0, 0.0), axis=1, keepdims=True)

    column = lanes[:, 0:128]
    tile_f = tiles[:, 0:128].astype(F32)
    upper = jnp.where(tile_f > 2.5, 1.0, 0.0)
    lower = jnp.where(tile_f < 1.5, 1.0, 0.0)
    table = jnp.zeros((BLOCKS, 128), F32)
    for group in range(GROUPS):
        start = below(float(ROWS * group))
        count = below(float(ROWS * group + ROWS + 5)) - start
        table = jnp.where(column == START + group, start, table)
        table = jnp.where(column == COUNT + group, count, table)
        table = jnp.where(column == COUNT + 8 + group, count * upper, table)
        table = jnp.where(column == COUNT + 16 + group, count * lower, table)
    count = below(5.0)
    table = jnp.where(column == WRAP, count, table)
    table = jnp.where(column == WRAP + 1, count * upper, table)
    table = jnp.where(column == WRAP + 2, count * lower, table)
    out_ref[TABLE : TABLE + BLOCKS, :] = table
    key = shifted * 256.0 + lanes.astype(F32)
    key_t = key.T
    place = lax.broadcasted_iota(I32, (256, 256), 0).astype(F32)
    for b in range(BLOCKS):
        before = key_t[:, b : b + 1] < key[b : b + 1, :]
        rank = jnp.sum(jnp.where(before, 1.0, 0.0), axis=0, keepdims=True)
        pick = jnp.where(place == rank, 1.0, 0.0).astype(BF16)
        rows = jnp.concatenate([fields[f * 8 + b : f * 8 + b + 1, :] for f in range(5)] + [jnp.zeros((3, 256), F32)], axis=0)
        top = rows.astype(BF16)
        rest = rows - top.astype(F32)
        mid = rest.astype(BF16)
        low = (rest - mid.astype(F32)).astype(BF16)
        parts = jnp.concatenate([top.astype(F32), mid.astype(F32), low.astype(F32)], axis=0).astype(BF16)
        moved = lax.dot_general(parts, pick, (((1,), (1,)), ((), ())), preferred_element_type=F32)
        ordered = (moved[0:8] + moved[8:16]) + moved[16:24]
        for f in range(FIELDS):
            for half in range(2):
                row = half * HALF_ROWS + f * 8 + b
                out_ref[row : row + 1, :] = ordered[f : f + 1, half * 128 : half * 128 + 128]


def exchange_kernel(tile_ref, count_ref, xy_ref, dz_ref, val_ref, out_ref, fields, own_ref, send_sem, recv_sem):
    grp = lax.axis_index("grp")
    slab = lax.axis_index("slab")
    far = lax.rem(grp + 4, 8)
    half = (grp // 4) * 4
    spot = grp - half
    peers = [half + lax.rem(spot + step, 4) for step in (1, 3, 2)]
    far_half = 4 - half
    up = lax.rem(slab + 1, 32)
    down = lax.rem(slab + 31, 32)
    around = [(far, slab)] + [(peer, slab) for peer in peers] + [(grp, up), (grp, down)]

    barrier = pltpu.get_barrier_semaphore()
    for device in around:
        pl.semaphore_signal(barrier, inc=1, device_id=device, device_id_type=MESH)
    sort_blocks(tile_ref, count_ref, xy_ref, dz_ref, val_ref, own_ref, fields)
    pl.semaphore_wait(barrier, len(around))

    sends = []

    def send(source, kind, owner, sem, device):
        copy = pltpu.make_async_remote_copy(
            src_ref=source,
            dst_ref=out_ref.at[kind, owner],
            send_sem=send_sem.at[len(sends)],
            recv_sem=recv_sem.at[sem],
            device_id=device,
            device_id_type=MESH,
        )
        copy.start()
        sends.append(copy)
        return copy

    def arrive(kind, owner, sem):
        pltpu.make_async_remote_copy(
            src_ref=own_ref,
            dst_ref=out_ref.at[kind, owner],
            send_sem=send_sem.at[0],
            recv_sem=recv_sem.at[sem],
            device_id=(grp, slab),
            device_id_type=MESH,
        ).wait_recv()

    send(own_ref, 0, grp, 0, (far, slab))
    for at, peer in enumerate(peers):
        send(own_ref, 0, grp, 1 + at, (peer, slab))
    send(own_ref, 1, grp, 7, (grp, up))
    send(own_ref, 2, grp, 15, (grp, down))
    out_ref[0, grp] = own_ref[...]
    back = [half + lax.rem(spot + step, 4) for step in (3, 1, 2)]
    for at in range(3):
        arrive(0, back[at], 1 + at)
        send(out_ref.at[0, back[at]], 1, back[at], 8 + at, (grp, up))
        send(out_ref.at[0, back[at]], 2, back[at], 16 + at, (grp, down))
    arrive(0, far, 0)
    for at, peer in enumerate(peers):
        send(out_ref.at[0, far], 0, far, 4 + at, (peer, slab))
    send(out_ref.at[0, far], 1, far, 11, (grp, up))
    send(out_ref.at[0, far], 2, far, 19, (grp, down))
    for at in range(3):
        owner = back[at] - half + far_half
        arrive(0, owner, 4 + at)
        send(out_ref.at[0, owner], 1, owner, 12 + at, (grp, up))
        send(out_ref.at[0, owner], 2, owner, 20 + at, (grp, down))
    for kind, base in ((1, 7), (2, 15)):
        arrive(kind, grp, base)
        arrive(kind, far, base + 4)
        for at in range(3):
            arrive(kind, back[at], base + 1 + at)
            arrive(kind, back[at] - half + far_half, base + 5 + at)
    for copy in sends:
        copy.wait_send()


def exchange(tile, count, xy, dz, val):
    vmem = pl.BlockSpec(memory_space=pltpu.VMEM)
    smem = pl.BlockSpec(memory_space=pltpu.SMEM)
    return pl.pallas_call(
        exchange_kernel,
        out_shape=jax.ShapeDtypeStruct((3, GROUPS, SEND_ROWS, 128), F32),
        in_specs=[smem, smem, vmem, vmem, vmem],
        out_specs=vmem,
        scratch_shapes=[
            pltpu.VMEM((HALF_ROWS, 256), F32),
            pltpu.VMEM((SEND_ROWS, 128), F32),
            pltpu.SemaphoreType.DMA((23,)),
            pltpu.SemaphoreType.DMA((23,)),
        ],
        compiler_params=pltpu.CompilerParams(collective_id=0, has_side_effects=True, vmem_limit_bytes=8 * 2**20),
        name="exchange",
    )(tile, count, xy, dz, val)


def grid_kernel(read_group, all_ref, out_ref, table_v, table, packed, lhs0, rhs0, lhs1, rhs1, total, flat, sem, out_sem):
    group = read_group()
    for source in range(SOURCES):
        first = source * SEND_ROWS + TABLE
        table_v[source * 8 : source * 8 + 8, :] = all_ref[first : first + 8, :].astype(I32)
    copy = pltpu.make_async_copy(table_v, table, sem)
    copy.start()
    total[...] = jnp.zeros_like(total)
    lhs1[...] = jnp.zeros_like(lhs1)
    rhs1[...] = jnp.zeros_like(rhs1)
    lanes = lax.broadcasted_iota(I32, (8, 128), 1)
    lanes_f = lanes[:FIELDS]
    subs = lax.broadcasted_iota(I32, (8, 128), 0)
    copy.wait()

    def append(kind, source, b, start, count, offset):
        first = source * SEND_ROWS + b
        low = lax.bitwise_and(start, 127)
        half = jnp.minimum(lax.shift_right_logical(start, 7), 1)
        values = all_ref[pl.ds(first + half * HALF_ROWS, FIELDS, stride=8), :]
        after = all_ref[pl.ds(first + HALF_ROWS, FIELDS, stride=8), :]
        values = jnp.where(lanes_f >= low, values, after)
        if kind > 0:
            values = values + jnp.where(subs[:FIELDS] == 2, (0.0, -6.0, 6.0)[kind], 0.0)
        at = lax.bitwise_and(offset, 127)
        rolled = pltpu.roll(values, lax.bitwise_and(at - low + 128, 127), 1)
        slot = lax.shift_right_logical(offset, 7)
        pltpu.store(packed.at[slot, 0:FIELDS], rolled, mask=lanes_f >= at)
        packed[slot + 1, 0:FIELDS] = rolled
        return offset + count

    def spans(kind, wrap, source, b):
        row = source * 8 + b
        if wrap:
            return 0, table[row, WRAP + kind]
        return table[row, group], table[row, COUNT + 8 * kind + group]

    def gather(kind, wrap, offset):
        def body(at, carry):
            offset, more = carry
            source = kind * GROUPS + at
            for b in range(BLOCKS):
                start, count = spans(kind, wrap, source, b)
                first = jnp.minimum(count, 128)
                offset = append(kind, source, b, start, first, offset)
                more = more + (count - first)
            return offset, more

        return body

    def gather_rest(kind, wrap):
        def body(at, offset):
            source = kind * GROUPS + lax.shift_right_logical(at, 3)
            b = lax.bitwise_and(at, 7)
            start, count = spans(kind, wrap, source, b)
            left = jnp.maximum(count - 128, 0)
            return lax.cond(left > 0, lambda o: append(kind, source, b, start + 128, left, o), lambda o: o, offset)

        return body

    offset = jnp.int32(0)
    for wrap in (False, True):
        for kind in range(3):
            steps = jnp.where(group == GROUPS - 1, GROUPS, 0) if wrap else GROUPS
            offset, more = lax.fori_loop(0, steps, gather(kind, wrap, offset), (offset, jnp.int32(0)))
            offset = lax.fori_loop(0, jnp.where(more > 0, 64, 0), gather_rest(kind, wrap), offset)

    subs_f = subs.astype(F32)
    first_row = (group * ROWS).astype(F32)

    def place(taps, base):
        away = subs_f - base
        part = -jnp.floor(away * 0.125)
        index = (away + 8.0 * part).astype(I32)
        turned = jnp.take_along_axis(taps, index, axis=0, mode="promise_in_bounds")
        part = jnp.where(part < 0.0, part + 48.0, part)
        part = jnp.where(part >= 48.0, part - 48.0, part)
        return turned, jnp.concatenate([part, part - 1.0], axis=0).astype(BF16)

    def twice(value):
        return jnp.concatenate([value, value], axis=0).astype(BF16)

    def build(lhs, rhs, at):
        for half in range(2):
            cols = slice(half * 128, half * 128 + 128)
            values = packed[at * 2 + half]
            values = jnp.where(lanes + (at * 256 + half * 128) < offset, values, 0.0)
            along_x, along_y, along_z = [jnp.broadcast_to(values[f : f + 1], (8, 128)) for f in range(3)]
            cell_x = jnp.floor(along_x)
            cell_y = jnp.floor(along_y)
            taps_x = kaiser(subs_f - 2.0 - (along_x - cell_x)).astype(BF16).astype(F32)
            taps_y = kaiser(subs_f - 2.0 - (along_y - cell_y))
            taps_z = kaiser(subs_f - along_z)
            turned_x, part_x = place(taps_x, cell_x - 2.0 - first_row)
            turned_y, part_y = place(taps_y, cell_y - 2.0)
            turned_y = twice(turned_y)
            zero = jnp.zeros((16, 128), BF16)
            for row in range(0, NY, 16):
                rhs[row : row + 16, cols] = jnp.where(part_y == row // 8, turned_y, zero)
            here = [part_x == row // 8 for row in range(0, ROWS, 16)]
            for z in range(PLANES):
                for c in range(2):
                    scale = jnp.broadcast_to(taps_z[z : z + 1] * values[3 + c : 4 + c], (8, 128))
                    scaled = twice(turned_x * scale)
                    for at_row, mask in enumerate(here):
                        first = (z * 2 + c) * ROWS + at_row * 16
                        lhs[first : first + 16, cols] = jnp.where(mask, scaled, zero)

    def multiply(lhs, rhs):
        total[...] += lax.dot_general(lhs[...], rhs[...], (((1,), (1,)), ((), ())), preferred_element_type=F32)

    def two_chunks(at, carry):
        build(lhs0, rhs0, at * 2)
        multiply(lhs1, rhs1)
        build(lhs1, rhs1, at * 2 + 1)
        multiply(lhs0, rhs0)
        return carry

    lax.fori_loop(0, lax.shift_right_logical(offset + 511, 9), two_chunks, 0)
    multiply(lhs1, rhs1)
    lines = flat.reshape(ROWS * PLANES * 6, 128)
    for z in range(PLANES):
        for c in range(2):
            for y in range(3):
                first = (z * 2 + c) * ROWS
                lines[pl.ds(z * 6 + y * 2 + c, ROWS, stride=36), :] = total[first : first + ROWS, y * 128 : y * 128 + 128]
    copies = [pltpu.make_async_copy(flat.at[:, y], out_ref.at[:, :, pl.ds(y * 128, 128)], out_sem.at[y]) for y in range(3)]
    for copy in copies:
        copy.start()
    for copy in copies:
        copy.wait()


def grid_block(everything, group=None):
    vmem = pl.BlockSpec(memory_space=pltpu.VMEM)
    if group is None:
        operands, specs = [everything], [vmem]

        def kernel(all_ref, *refs):
            grid_kernel(lambda: lax.axis_index("grp"), all_ref, *refs)
    else:
        operands, specs = [group, everything], [pl.BlockSpec(memory_space=pltpu.SMEM), vmem]

        def kernel(group_ref, all_ref, *refs):
            grid_kernel(lambda: group_ref[0], all_ref, *refs)

    return pl.pallas_call(
        kernel,
        out_shape=jax.ShapeDtypeStruct((ROWS * PLANES, 2, NY), F32),
        in_specs=specs,
        out_specs=pl.BlockSpec(memory_space=pl.ANY),
        scratch_shapes=[
            pltpu.VMEM((SOURCES * 8, 128), I32),
            pltpu.SMEM((SOURCES * 8, 128), I32),
            pltpu.VMEM((388, 8, 128), F32),
            pltpu.VMEM((12 * ROWS, 256), BF16),
            pltpu.VMEM((NY, 256), BF16),
            pltpu.VMEM((12 * ROWS, 256), BF16),
            pltpu.VMEM((NY, 256), BF16),
            pltpu.VMEM((12 * ROWS, NY), F32),
            pltpu.VMEM((ROWS * PLANES, 3, 2, 128), F32),
            pltpu.SemaphoreType.DMA,
            pltpu.SemaphoreType.DMA((3,)),
        ],
        compiler_params=pltpu.CompilerParams(vmem_limit_bytes=16 * 2**20),
        name="grid_block",
    )(*operands)


def shards(sample_xy, sample_dz, sample_values, block_tile, block_count):
    everything = exchange(
        block_tile, block_count, sample_xy.reshape(8, 2, 256), sample_dz.reshape(8, 256), sample_values.reshape(8, 2, 256)
    )
    block = grid_block(everything.reshape(SOURCES * SEND_ROWS, 128))
    return block.reshape(ROWS, PLANES, 2, NY)


def solution(mesh):
    return jax.shard_map(
        shards,
        mesh=mesh,
        in_specs=(
            P("grp", "slab", None, None, None),
            P("grp", "slab", None, None),
            P("grp", "slab", None, None, None),
            P("grp", "slab", None),
            P("grp", "slab", None),
        ),
        out_specs=P("grp", "slab", None, None),
        check_vma=False,
    )
```

```python
import math

import jax
import jax.numpy as jnp
from jax import lax
from jax.experimental import pallas as pl
from jax.experimental.pallas import tpu as pltpu
from jax.sharding import PartitionSpec as P

NX = 384
NY = 384
PLANES = 6
BLOCKS = 8
GROUPS = 8
ROWS = 48
FIELDS = 5
HALF_ROWS = FIELDS * BLOCKS
TABLE = 2 * HALF_ROWS
SEND_ROWS = TABLE + BLOCKS
SOURCES = 3 * GROUPS
START, COUNT, LEFT, WRAP, WRAP_LEFT, ANY_LEFT = 0, 8, 32, 56, 80, 104
MESH = pl.DeviceIdType.MESH
BETA = math.pi * math.sqrt(19.45)
F32 = jnp.float32
BF16 = jnp.bfloat16
I32 = jnp.int32


def kaiser_coefficients():
    half_sq = (0.5 * BETA) ** 2
    terms = []
    term = 1.0
    for order in range(1, 32):
        term = term * half_sq / (order * order)
        terms.append(term)
    top = sum(terms)
    return [value / top for value in terms]


COEFF = kaiser_coefficients()


def kaiser(distance):
    third = distance * (1.0 / 3.0)
    inside = jnp.maximum(1.0 - third * third, 0.0)
    square = inside * inside
    fourth = square * square
    chains = []
    for first in range(4):
        picked = COEFF[first::4]
        total = jnp.full_like(inside, picked[-1])
        for value in picked[-2::-1]:
            total = total * fourth + value
        chains.append(total)
    low = chains[0] + chains[1] * inside
    high = chains[2] + chains[3] * inside
    return (low + high * square) * inside


def sort_blocks(tile_ref, count_ref, xy_ref, dz_ref, val_ref, out_ref, fields):
    lanes = lax.broadcasted_iota(I32, (BLOCKS, 256), 1)
    subs = lax.broadcasted_iota(I32, (BLOCKS, 256), 0)
    counts = jnp.zeros((BLOCKS, 256), I32)
    tiles = jnp.zeros((BLOCKS, 256), I32)
    for b in range(BLOCKS):
        counts = jnp.where(subs == b, count_ref[0, 0, b], counts)
        tiles = jnp.where(subs == b, tile_ref[0, 0, b], tiles)
    along_x = xy_ref[:, 0, :]
    cell = jnp.floor(along_x)
    shifted = cell + 3.0
    shifted = jnp.where(shifted >= NX, shifted - NX, shifted)
    shifted = jnp.where(lanes < counts, shifted, 400.0)
    fields[0:8] = along_x
    fields[8:16] = xy_ref[:, 1, :]
    fields[16:24] = dz_ref[...] + tiles.astype(F32)
    fields[24:32] = val_ref[:, 0, :]
    fields[32:40] = val_ref[:, 1, :]

    def below(bound):
        return jnp.sum(jnp.where(shifted < bound, 1.0, 0.0), axis=1, keepdims=True)

    column = lanes[:, 0:128]
    tile_f = tiles[:, 0:128].astype(F32)
    kinds = [jnp.ones((BLOCKS, 128), F32), jnp.where(tile_f > 2.5, 1.0, 0.0), jnp.where(tile_f < 1.5, 1.0, 0.0)]
    table = jnp.zeros((BLOCKS, 128), F32)
    for group in range(GROUPS):
        start = below(float(ROWS * group))
        count = below(float(ROWS * group + ROWS + 5)) - start
        first = jnp.minimum(count, 128.0)
        table = jnp.where(column == START + group, jnp.minimum(start, 255.0), table)
        for kind in range(3):
            table = jnp.where(column == COUNT + 8 * kind + group, first * kinds[kind], table)
            table = jnp.where(column == LEFT + 8 * kind + group, (count - first) * kinds[kind], table)
    count = below(5.0)
    first = jnp.minimum(count, 128.0)
    for kind in range(3):
        table = jnp.where(column == WRAP + kind, first * kinds[kind], table)
        table = jnp.where(column == WRAP + 3 + kind, (count - first) * kinds[kind], table)
    table = table.T
    pieces = [table[at : at + 8] for at in range(0, WRAP, 8)]
    pieces += [jnp.broadcast_to(table[WRAP + at : WRAP + at + 1], (8, 8)) for at in range(6)]
    left = pieces[4] + pieces[10]
    pieces.append(jnp.broadcast_to(jnp.sum(left, axis=1, keepdims=True), (8, 8)))
    out_ref[TABLE : TABLE + BLOCKS, :] = jnp.concatenate(pieces + [jnp.zeros((8, 128 - 8 * len(pieces)), F32)], axis=1)
    key = shifted * 256.0 + lanes.astype(F32)
    key_t = key.T
    place = lax.broadcasted_iota(I32, (256, 256), 0).astype(F32)
    for b in range(BLOCKS):
        before = key_t[:, b : b + 1] < key[b : b + 1, :]
        rank = jnp.sum(jnp.where(before, 1.0, 0.0), axis=0, keepdims=True)
        pick = jnp.where(place == rank, 1.0, 0.0).astype(BF16)
        rows = jnp.concatenate([fields[f * 8 + b : f * 8 + b + 1, :] for f in range(5)] + [jnp.zeros((3, 256), F32)], axis=0)
        top = rows.astype(BF16)
        rest = rows - top.astype(F32)
        mid = rest.astype(BF16)
        low = (rest - mid.astype(F32)).astype(BF16)
        parts = jnp.concatenate([top.astype(F32), mid.astype(F32), low.astype(F32)], axis=0).astype(BF16)
        moved = lax.dot_general(parts, pick, (((1,), (1,)), ((), ())), preferred_element_type=F32)
        ordered = (moved[0:8] + moved[8:16]) + moved[16:24]
        for f in range(FIELDS):
            for half in range(2):
                row = half * HALF_ROWS + f * 8 + b
                out_ref[row : row + 1, :] = ordered[f : f + 1, half * 128 : half * 128 + 128]


def exchange_kernel(
    tile_in, count_in, xy_in, dz_in, val_in, out_ref, tile_ref, count_ref, xy_ref, dz_ref, val_ref, fields, own_ref, in_sem, send_sem, recv_sem
):
    loads = [
        pltpu.make_async_copy(source, target, in_sem.at[at])
        for at, (source, target) in enumerate(
            [(xy_in, xy_ref), (tile_in, tile_ref), (count_in, count_ref), (dz_in, dz_ref), (val_in, val_ref)]
        )
    ]
    for load in loads:
        load.start()
    grp = lax.axis_index("grp")
    slab = lax.axis_index("slab")
    far = lax.rem(grp + 4, 8)
    half = (grp // 4) * 4
    spot = grp - half
    peers = [half + lax.rem(spot + step, 4) for step in (2, 1, 3)]
    far_half = 4 - half
    up = lax.rem(slab + 1, 32)
    down = lax.rem(slab + 31, 32)
    around = [(far, slab)] + [(peer, slab) for peer in peers] + [(grp, up), (grp, down)]

    barrier = pltpu.get_barrier_semaphore()
    for device in around:
        pl.semaphore_signal(barrier, inc=1, device_id=device, device_id_type=MESH)
    for load in loads:
        load.wait()
    sort_blocks(tile_ref, count_ref, xy_ref, dz_ref, val_ref, own_ref, fields)
    pl.semaphore_wait(barrier, len(around))

    sends = []

    def send(source, kind, owner, sem, device):
        copy = pltpu.make_async_remote_copy(
            src_ref=source,
            dst_ref=out_ref.at[kind, owner],
            send_sem=send_sem.at[len(sends)],
            recv_sem=recv_sem.at[sem],
            device_id=device,
            device_id_type=MESH,
        )
        copy.start()
        sends.append(copy)
        return copy

    def arrive(kind, owner, sem):
        pltpu.make_async_remote_copy(
            src_ref=own_ref,
            dst_ref=out_ref.at[kind, owner],
            send_sem=send_sem.at[0],
            recv_sem=recv_sem.at[sem],
            device_id=(grp, slab),
            device_id_type=MESH,
        ).wait_recv()

    send(own_ref, 0, grp, 0, (far, slab))
    for at, peer in enumerate(peers):
        send(own_ref, 0, grp, 1 + at, (peer, slab))
    send(own_ref, 1, grp, 7, (grp, up))
    send(own_ref, 2, grp, 15, (grp, down))
    out_ref[0, grp] = own_ref[...]
    back = [half + lax.rem(spot + step, 4) for step in (2, 3, 1)]
    for at in range(3):
        arrive(0, back[at], 1 + at)
        send(out_ref.at[0, back[at]], 1, back[at], 8 + at, (grp, up))
        send(out_ref.at[0, back[at]], 2, back[at], 16 + at, (grp, down))
    arrive(0, far, 0)
    for at, peer in enumerate(peers):
        send(out_ref.at[0, far], 0, far, 4 + at, (peer, slab))
    send(out_ref.at[0, far], 1, far, 11, (grp, up))
    send(out_ref.at[0, far], 2, far, 19, (grp, down))
    for at in range(3):
        owner = back[at] - half + far_half
        arrive(0, owner, 4 + at)
        send(out_ref.at[0, owner], 1, owner, 12 + at, (grp, up))
        send(out_ref.at[0, owner], 2, owner, 20 + at, (grp, down))
    for kind, base in ((1, 7), (2, 15)):
        arrive(kind, grp, base)
        arrive(kind, far, base + 4)
        for at in range(3):
            arrive(kind, back[at], base + 1 + at)
            arrive(kind, back[at] - half + far_half, base + 5 + at)
    for copy in sends:
        copy.wait_send()


def exchange(tile, count, xy, dz, val):
    vmem = pl.BlockSpec(memory_space=pltpu.VMEM)
    hbm = pl.BlockSpec(memory_space=pltpu.HBM)
    return pl.pallas_call(
        exchange_kernel,
        out_shape=jax.ShapeDtypeStruct((3, GROUPS, SEND_ROWS, 128), F32),
        in_specs=[hbm] * 5,
        out_specs=vmem,
        scratch_shapes=[
            pltpu.SMEM((1, 1, 8), I32),
            pltpu.SMEM((1, 1, 8), I32),
            pltpu.VMEM((BLOCKS, 2, 256), F32),
            pltpu.VMEM((BLOCKS, 256), F32),
            pltpu.VMEM((BLOCKS, 2, 256), F32),
            pltpu.VMEM((HALF_ROWS, 256), F32),
            pltpu.VMEM((SEND_ROWS, 128), F32),
            pltpu.SemaphoreType.DMA((5,)),
            pltpu.SemaphoreType.DMA((23,)),
            pltpu.SemaphoreType.DMA((23,)),
        ],
        compiler_params=pltpu.CompilerParams(collective_id=0, has_side_effects=True, vmem_limit_bytes=8 * 2**20),
        name="exchange",
    )(tile, count, xy, dz, val)


def grid_kernel(read_group, all_ref, out_ref, table_v, table, packed, held0, held1, flat, sem, out_sem):
    group = read_group()
    for source in range(SOURCES):
        table_v[source : source + 1, :] = all_ref[pl.ds(source * SEND_ROWS + TABLE + group, 1), :].astype(I32)
    copy = pltpu.make_async_copy(table_v, table, sem)
    copy.start()
    lanes = lax.broadcasted_iota(I32, (8, 128), 1)
    lanes_f = lanes[:FIELDS]
    subs = lax.broadcasted_iota(I32, (8, 128), 0)
    copy.wait()

    def append(kind, source, b, start, count, offset):
        first = source * SEND_ROWS + b
        low = lax.bitwise_and(start, 127)
        half = lax.shift_right_logical(start, 7)
        values = all_ref[pl.ds(first + half * HALF_ROWS, FIELDS, stride=8), :]
        after = all_ref[pl.ds(first + HALF_ROWS, FIELDS, stride=8), :]
        values = jnp.where(lanes_f >= low, values, after)
        if kind > 0:
            values = values + jnp.where(subs[:FIELDS] == 2, (0.0, -6.0, 6.0)[kind], 0.0)
        at = lax.bitwise_and(offset, 127)
        rolled = pltpu.roll(values, lax.bitwise_and(at - low, 127), 1)
        slot = lax.shift_right_logical(offset, 7)
        pltpu.store(packed.at[slot, 0:FIELDS], rolled, mask=lanes_f >= at)
        packed[slot + 1, 0:FIELDS] = rolled
        return offset + count

    def gather(kind, wrap):
        def body(at, carry):
            offset, more = carry
            source = kind * GROUPS + at
            for b in range(BLOCKS):
                start = jnp.int32(0) if wrap else table[source, START + b]
                offset = append(kind, source, b, start, table[source, (WRAP if wrap else COUNT) + 8 * kind + b], offset)
            return offset, more + table[source, ANY_LEFT]

        return body

    def gather_rest(kind, wrap):
        def body(at, offset):
            source = kind * GROUPS + lax.shift_right_logical(at, 3)
            b = lax.bitwise_and(at, 7)
            start = jnp.int32(0) if wrap else table[source, START + b]
            left = table[source, (WRAP_LEFT if wrap else LEFT) + 8 * kind + b]
            return lax.cond(left > 0, lambda o: append(kind, source, b, start + 128, left, o), lambda o: o, offset)

        return body

    offset = jnp.int32(0)
    for wrap in (False, True):
        for kind in range(3):
            steps = jnp.where(group == GROUPS - 1, GROUPS, 0) if wrap else GROUPS
            offset, more = lax.fori_loop(0, steps, gather(kind, wrap), (offset, jnp.int32(0)))
            offset = lax.fori_loop(0, jnp.where(more > 0, 64, 0), gather_rest(kind, wrap), offset)

    subs_f = subs.astype(F32)
    first_row = (group * ROWS).astype(F32)

    def place(taps, base):
        away = subs_f - base
        part = -jnp.floor(away * 0.125)
        index = (away + 8.0 * part).astype(I32)
        turned = jnp.take_along_axis(taps, index, axis=0, mode="promise_in_bounds")
        part = jnp.where(part < 0.0, part + 48.0, part)
        part = jnp.where(part >= 48.0, part - 48.0, part)
        return turned, part

    def pair(part):
        return jnp.concatenate([part, part - 1.0], axis=0).astype(BF16)

    def twice(value):
        return jnp.concatenate([value, value], axis=0).astype(BF16)

    zero = jnp.zeros((16, 128), BF16)

    def prepare(held, at):
        sides = []
        for half in range(2):
            values = packed[at * 2 + half]
            values = jnp.where(lanes + (at * 256 + half * 128) < offset, values, 0.0)
            along_x, along_y, along_z = [jnp.broadcast_to(values[f : f + 1], (8, 128)) for f in range(3)]
            cell_x = jnp.floor(along_x)
            cell_y = jnp.floor(along_y)
            taps_x = kaiser(subs_f - 2.0 - (along_x - cell_x)).astype(BF16).astype(F32)
            taps_y = kaiser(subs_f - 2.0 - (along_y - cell_y))
            taps_z = kaiser(subs_f - along_z)
            turned_x, part_x = place(taps_x, cell_x - 2.0 - first_row)
            turned_y, part_y = place(taps_y, cell_y - 2.0)
            held[half, 0] = turned_x
            held[half, 1] = part_x
            for c in range(2):
                held[half, 2 + c] = taps_z * jnp.broadcast_to(values[3 + c : 4 + c], (8, 128))
            turned_y, part_y = twice(turned_y), pair(part_y)
            sides.append([jnp.where(part_y == group_y, turned_y, zero) for group_y in range(0, NY // 8, 2)] + [zero] * 8)
        for unit in range(2):
            tiles = [jnp.concatenate([side[unit * 16 + at] for side in sides], axis=1) for at in range(16)]
            pltpu.matmul_push_rhs(jnp.concatenate(tiles, axis=0), staging_register=0, mxu_index=unit, transpose=True)

    def stream(held, sums):
        here = []
        for half in range(2):
            part_x = pair(held[half, 1])
            here.append([part_x == group_x for group_x in range(0, ROWS // 8, 2)])
        for plane in range(2 * PLANES):
            z, c = plane // 2, plane % 2
            sides = []
            for half in range(2):
                scaled = twice(held[half, 0] * jnp.broadcast_to(held[half, 2 + c, z : z + 1], (8, 128)))
                sides.append([jnp.where(mask, scaled, zero) for mask in here[half]])
            rows = jnp.concatenate([jnp.concatenate([side[at] for side in sides], axis=1) for at in range(3)], axis=0)
            for unit in range(2):
                pltpu.matmul_acc_lhs(sums[unit][plane], rows, load_staged_rhs=0 if plane == 0 else None)

    def run(*accumulators):
        sums = (accumulators[:12], accumulators[12:])
        prepare(held0, 0)

        def two_chunks(at, carry):
            stream(held0, sums)
            prepare(held1, at * 2 + 1)
            stream(held1, sums)
            prepare(held0, at * 2 + 2)
            return carry

        lax.fori_loop(0, lax.shift_right_logical(offset + 511, 9), two_chunks, 0)
        for unit in range(2):
            pltpu.matmul_acc_lhs(sums[unit][0], jnp.zeros((ROWS, 256), BF16), load_staged_rhs=0)
        lines = flat.reshape(ROWS * PLANES * 6, 128)
        for plane in range(2 * PLANES):
            z, c = plane // 2, plane % 2
            sides = [pltpu.matmul_pop(sums[unit][plane]) for unit in range(2)]
            for y in range(3):
                lines[pl.ds(z * 6 + y * 2 + c, ROWS, stride=36), :] = sides[y // 2][:, (y % 2) * 128 : (y % 2) * 128 + 128]

    pl.run_scoped(run, *[pltpu.ACC(unit)((ROWS, 256), F32) for unit in range(2) for _ in range(12)])
    copies = [pltpu.make_async_copy(flat.at[:, y], out_ref.at[:, :, pl.ds(y * 128, 128)], out_sem.at[y]) for y in range(3)]
    for copy in copies:
        copy.start()
    for copy in copies:
        copy.wait()


def grid_block(everything, group=None):
    vmem = pl.BlockSpec(memory_space=pltpu.VMEM)
    if group is None:
        operands, specs = [everything], [vmem]

        def kernel(all_ref, *refs):
            grid_kernel(lambda: lax.axis_index("grp"), all_ref, *refs)
    else:
        operands, specs = [group, everything], [pl.BlockSpec(memory_space=pltpu.SMEM), vmem]

        def kernel(group_ref, all_ref, *refs):
            grid_kernel(lambda: group_ref[0], all_ref, *refs)

    return pl.pallas_call(
        kernel,
        out_shape=jax.ShapeDtypeStruct((ROWS * PLANES, 2, NY), F32),
        in_specs=specs,
        out_specs=pl.BlockSpec(memory_space=pl.ANY),
        scratch_shapes=[
            pltpu.VMEM((SOURCES, 128), I32),
            pltpu.SMEM((SOURCES, 128), I32),
            pltpu.VMEM((388, 8, 128), F32),
            pltpu.VMEM((2, 4, 8, 128), F32),
            pltpu.VMEM((2, 4, 8, 128), F32),
            pltpu.VMEM((ROWS * PLANES, 3, 2, 128), F32),
            pltpu.SemaphoreType.DMA,
            pltpu.SemaphoreType.DMA((3,)),
        ],
        compiler_params=pltpu.CompilerParams(vmem_limit_bytes=16 * 2**20),
        name="grid_block",
    )(*operands)


def shards(sample_xy, sample_dz, sample_values, block_tile, block_count):
    operands = [block_tile, block_count, sample_xy.reshape(8, 2, 256), sample_dz.reshape(8, 256), sample_values.reshape(8, 2, 256)]
    everything = exchange(*[pltpu.with_memory_space_constraint(operand, pltpu.HBM) for operand in operands])
    block = grid_block(everything.reshape(SOURCES * SEND_ROWS, 128))
    return block.reshape(ROWS, PLANES, 2, NY)


def solution(mesh):
    return jax.shard_map(
        shards,
        mesh=mesh,
        in_specs=(
            P("grp", "slab", None, None, None),
            P("grp", "slab", None, None),
            P("grp", "slab", None, None, None),
            P("grp", "slab", None),
            P("grp", "slab", None),
        ),
        out_specs=P("grp", "slab", None, None),
        check_vma=False,
    )
```

```python
import math

import jax
import jax.numpy as jnp
from jax import lax
from jax.experimental import pallas as pl
from jax.experimental.pallas import tpu as pltpu
from jax.sharding import PartitionSpec as P

NX = 384
NY = 384
PLANES = 6
BLOCKS = 8
GROUPS = 8
ROWS = 48
FIELDS = 5
HALF_ROWS = FIELDS * BLOCKS
TABLE = 2 * HALF_ROWS
SEND_ROWS = TABLE + BLOCKS
SOURCES = 3 * GROUPS
START, COUNT, LEFT, WRAP, WRAP_LEFT, ANY_LEFT = 0, 8, 32, 56, 80, 104
MESH = pl.DeviceIdType.MESH
BETA = math.pi * math.sqrt(19.45)
F32 = jnp.float32
BF16 = jnp.bfloat16
I32 = jnp.int32


def kaiser_coefficients():
    half_sq = (0.5 * BETA) ** 2
    terms = []
    term = 1.0
    for order in range(1, 32):
        term = term * half_sq / (order * order)
        terms.append(term)
    top = sum(terms)
    return [value / top for value in terms]


COEFF = kaiser_coefficients()


def kaiser(distance):
    third = distance * (1.0 / 3.0)
    inside = jnp.maximum(1.0 - third * third, 0.0)
    square = inside * inside
    fourth = square * square
    chains = []
    for first in range(4):
        picked = COEFF[first::4]
        total = jnp.full_like(inside, picked[-1])
        for value in picked[-2::-1]:
            total = total * fourth + value
        chains.append(total)
    low = chains[0] + chains[1] * inside
    high = chains[2] + chains[3] * inside
    return (low + high * square) * inside


def sort_blocks(tile_ref, count_ref, xy_ref, dz_ref, val_ref, out_ref, fields):
    lanes = lax.broadcasted_iota(I32, (BLOCKS, 256), 1)
    subs = lax.broadcasted_iota(I32, (BLOCKS, 256), 0)
    counts = jnp.zeros((BLOCKS, 256), I32)
    tiles = jnp.zeros((BLOCKS, 256), I32)
    for b in range(BLOCKS):
        counts = jnp.where(subs == b, count_ref[0, 0, b], counts)
        tiles = jnp.where(subs == b, tile_ref[0, 0, b], tiles)
    along_x = xy_ref[:, 0, :]
    cell = jnp.floor(along_x)
    shifted = cell + 3.0
    shifted = jnp.where(shifted >= NX, shifted - NX, shifted)
    shifted = jnp.where(lanes < counts, shifted, 400.0)
    fields[0:8] = along_x
    fields[8:16] = xy_ref[:, 1, :]
    fields[16:24] = dz_ref[...] + tiles.astype(F32)
    fields[24:32] = val_ref[:, 0, :]
    fields[32:40] = val_ref[:, 1, :]

    def below(bound):
        return jnp.sum(jnp.where(shifted < bound, 1.0, 0.0), axis=1, keepdims=True)

    column = lanes[:, 0:128]
    tile_f = tiles[:, 0:128].astype(F32)
    kinds = [jnp.ones((BLOCKS, 128), F32), jnp.where(tile_f > 2.5, 1.0, 0.0), jnp.where(tile_f < 1.5, 1.0, 0.0)]
    table = jnp.zeros((BLOCKS, 128), F32)
    for group in range(GROUPS):
        start = below(float(ROWS * group))
        count = below(float(ROWS * group + ROWS + 5)) - start
        first = jnp.minimum(count, 128.0)
        table = jnp.where(column == START + group, jnp.minimum(start, 255.0), table)
        for kind in range(3):
            table = jnp.where(column == COUNT + 8 * kind + group, first * kinds[kind], table)
            table = jnp.where(column == LEFT + 8 * kind + group, (count - first) * kinds[kind], table)
    count = below(5.0)
    first = jnp.minimum(count, 128.0)
    for kind in range(3):
        table = jnp.where(column == WRAP + kind, first * kinds[kind], table)
        table = jnp.where(column == WRAP + 3 + kind, (count - first) * kinds[kind], table)
    table = table.T
    pieces = [table[at : at + 8] for at in range(0, WRAP, 8)]
    pieces += [jnp.broadcast_to(table[WRAP + at : WRAP + at + 1], (8, 8)) for at in range(6)]
    left = pieces[4] + pieces[10]
    pieces.append(jnp.broadcast_to(jnp.sum(left, axis=1, keepdims=True), (8, 8)))
    out_ref[TABLE : TABLE + BLOCKS, :] = jnp.concatenate(pieces + [jnp.zeros((8, 128 - 8 * len(pieces)), F32)], axis=1)
    key = shifted * 256.0 + lanes.astype(F32)
    key_t = key.T
    place = lax.broadcasted_iota(I32, (256, 256), 0).astype(F32)
    for b in range(BLOCKS):
        before = key_t[:, b : b + 1] < key[b : b + 1, :]
        rank = jnp.sum(jnp.where(before, 1.0, 0.0), axis=0, keepdims=True)
        pick = jnp.where(place == rank, 1.0, 0.0).astype(BF16)
        rows = jnp.concatenate([fields[f * 8 + b : f * 8 + b + 1, :] for f in range(5)] + [jnp.zeros((3, 256), F32)], axis=0)
        top = rows.astype(BF16)
        rest = rows - top.astype(F32)
        mid = rest.astype(BF16)
        low = (rest - mid.astype(F32)).astype(BF16)
        parts = jnp.concatenate([top.astype(F32), mid.astype(F32), low.astype(F32)], axis=0).astype(BF16)
        moved = lax.dot_general(parts, pick, (((1,), (1,)), ((), ())), preferred_element_type=F32)
        ordered = (moved[0:8] + moved[8:16]) + moved[16:24]
        for f in range(FIELDS):
            for half in range(2):
                row = half * HALF_ROWS + f * 8 + b
                out_ref[row : row + 1, :] = ordered[f : f + 1, half * 128 : half * 128 + 128]


def exchange_kernel(
    tile_in, count_in, xy_in, dz_in, val_in, out_ref, tile_ref, count_ref, xy_ref, dz_ref, val_ref, fields, own_ref, in_sem, send_sem, recv_sem
):
    loads = [
        pltpu.make_async_copy(source, target, in_sem.at[at])
        for at, (source, target) in enumerate(
            [(xy_in, xy_ref), (tile_in, tile_ref), (count_in, count_ref), (dz_in, dz_ref), (val_in, val_ref)]
        )
    ]
    for load in loads:
        load.start()
    grp = lax.axis_index("grp")
    slab = lax.axis_index("slab")
    far = lax.rem(grp + 4, 8)
    half = (grp // 4) * 4
    spot = grp - half
    peers = [half + lax.rem(spot + step, 4) for step in (2, 1, 3)]
    far_half = 4 - half
    core = lax.rem(slab, 2)
    outer = lax.rem(slab + 31 - 30 * core, 32)
    inner = lax.rem(slab + 1 + 30 * core, 32)
    beside = [((grp, outer), 2 - core), ((grp, inner), 1 + core)]
    around = [(far, slab)] + [(peer, slab) for peer in peers] + [(grp, outer), (grp, inner)]

    barrier = pltpu.get_barrier_semaphore()
    for device in around:
        pl.semaphore_signal(barrier, inc=1, device_id=device, device_id_type=MESH)
    for load in loads:
        load.wait()
    sort_blocks(tile_ref, count_ref, xy_ref, dz_ref, val_ref, own_ref, fields)
    pl.semaphore_wait(barrier, len(around))

    sends = []

    def rows_of(ref, rows):
        return ref if rows is None else ref.at[pl.ds(rows[0], rows[1])]

    def send(source, kind, owner, item, device, rows=None):
        copy = pltpu.make_async_remote_copy(
            src_ref=rows_of(source, rows),
            dst_ref=rows_of(out_ref.at[kind, owner], rows),
            send_sem=send_sem.at[len(sends)],
            recv_sem=recv_sem.at[kind, item],
            device_id=device,
            device_id_type=MESH,
        )
        copy.start()
        sends.append(copy)

    def arrive(kind, owner, item, rows=None):
        pltpu.make_async_remote_copy(
            src_ref=rows_of(own_ref, rows),
            dst_ref=rows_of(out_ref.at[kind, owner], rows),
            send_sem=send_sem.at[0],
            recv_sem=recv_sem.at[kind, item],
            device_id=(grp, slab),
            device_id_type=MESH,
        ).wait_recv()

    pieces = [(0, HALF_ROWS), (HALF_ROWS, SEND_ROWS - HALF_ROWS)]
    for at, rows in enumerate(pieces):
        send(own_ref, 0, grp, 4 + at, (far, slab), rows)
    for at, peer in enumerate(peers):
        send(own_ref, 0, grp, 1 + at, (peer, slab))
    for device, kind in beside:
        send(own_ref, kind, grp, 0, device)
    out_ref[0, grp] = own_ref[...]
    back = [half + lax.rem(spot + step, 4) for step in (2, 3, 1)]
    for at in range(3):
        arrive(0, back[at], 1 + at)
        for device, kind in beside:
            send(out_ref.at[0, back[at]], kind, back[at], 1 + at, device)
    for piece, rows in enumerate(pieces):
        arrive(0, far, 4 + piece, rows)
        for at, peer in enumerate(peers):
            send(out_ref.at[0, far], 0, far, 6 + 2 * at + piece, (peer, slab), rows)
        for device, kind in beside:
            send(out_ref.at[0, far], kind, far, 4 + piece, device, rows)
    for piece, rows in enumerate(pieces):
        for at in range(3):
            owner = back[at] - half + far_half
            arrive(0, owner, 6 + 2 * at + piece, rows)
            for device, kind in beside:
                send(out_ref.at[0, owner], kind, owner, 6 + 2 * at + piece, device, rows)
    for kind in (1, 2):
        arrive(kind, grp, 0)
        for at in range(3):
            arrive(kind, back[at], 1 + at)
        for piece, rows in enumerate(pieces):
            arrive(kind, far, 4 + piece, rows)
            for at in range(3):
                arrive(kind, back[at] - half + far_half, 6 + 2 * at + piece, rows)
    for copy in sends:
        copy.wait_send()


def exchange(tile, count, xy, dz, val):
    vmem = pl.BlockSpec(memory_space=pltpu.VMEM)
    hbm = pl.BlockSpec(memory_space=pltpu.HBM)
    return pl.pallas_call(
        exchange_kernel,
        out_shape=jax.ShapeDtypeStruct((3, GROUPS, SEND_ROWS, 128), F32),
        in_specs=[hbm] * 5,
        out_specs=vmem,
        scratch_shapes=[
            pltpu.SMEM((1, 1, 8), I32),
            pltpu.SMEM((1, 1, 8), I32),
            pltpu.VMEM((BLOCKS, 2, 256), F32),
            pltpu.VMEM((BLOCKS, 256), F32),
            pltpu.VMEM((BLOCKS, 2, 256), F32),
            pltpu.VMEM((HALF_ROWS, 256), F32),
            pltpu.VMEM((SEND_ROWS, 128), F32),
            pltpu.SemaphoreType.DMA((5,)),
            pltpu.SemaphoreType.DMA((35,)),
            pltpu.SemaphoreType.DMA((3, 12)),
        ],
        compiler_params=pltpu.CompilerParams(collective_id=0, has_side_effects=True, vmem_limit_bytes=8 * 2**20),
        name="exchange",
    )(tile, count, xy, dz, val)


def grid_kernel(read_group, all_ref, out_ref, table_v, table, packed, held0, held1, flat, sem, out_sem):
    group = read_group()
    for source in range(SOURCES):
        table_v[source : source + 1, :] = all_ref[pl.ds(source * SEND_ROWS + TABLE + group, 1), :].astype(I32)
    copy = pltpu.make_async_copy(table_v, table, sem)
    copy.start()
    lanes = lax.broadcasted_iota(I32, (8, 128), 1)
    lanes_f = lanes[:FIELDS]
    subs = lax.broadcasted_iota(I32, (8, 128), 0)
    copy.wait()

    def append(kind, source, b, start, count, offset):
        first = source * SEND_ROWS + b
        low = lax.bitwise_and(start, 127)
        half = lax.shift_right_logical(start, 7)
        values = all_ref[pl.ds(first + half * HALF_ROWS, FIELDS, stride=8), :]
        after = all_ref[pl.ds(first + HALF_ROWS, FIELDS, stride=8), :]
        values = jnp.where(lanes_f >= low, values, after)
        if kind > 0:
            values = values + jnp.where(subs[:FIELDS] == 2, (0.0, -6.0, 6.0)[kind], 0.0)
        at = lax.bitwise_and(offset, 127)
        rolled = pltpu.roll(values, lax.bitwise_and(at - low, 127), 1)
        slot = lax.shift_right_logical(offset, 7)
        pltpu.store(packed.at[slot, 0:FIELDS], rolled, mask=lanes_f >= at)
        packed[slot + 1, 0:FIELDS] = rolled
        return offset + count

    def gather(kind, wrap):
        def body(at, carry):
            offset, more = carry
            source = kind * GROUPS + at
            for b in range(BLOCKS):
                start = jnp.int32(0) if wrap else table[source, START + b]
                offset = append(kind, source, b, start, table[source, (WRAP if wrap else COUNT) + 8 * kind + b], offset)
            return offset, more + table[source, ANY_LEFT]

        return body

    def gather_rest(kind, wrap):
        def body(at, offset):
            source = kind * GROUPS + lax.shift_right_logical(at, 3)
            b = lax.bitwise_and(at, 7)
            start = jnp.int32(0) if wrap else table[source, START + b]
            left = table[source, (WRAP_LEFT if wrap else LEFT) + 8 * kind + b]
            return lax.cond(left > 0, lambda o: append(kind, source, b, start + 128, left, o), lambda o: o, offset)

        return body

    offset = jnp.int32(0)
    for kind in range(3):
        more = jnp.int32(0)
        for at in range(GROUPS):
            offset, more = gather(kind, False)(at, (offset, more))
        offset = lax.fori_loop(0, jnp.where(more > 0, 64, 0), gather_rest(kind, False), offset)
    for kind in range(3):
        steps = jnp.where(group == GROUPS - 1, GROUPS, 0)
        offset, more = lax.fori_loop(0, steps, gather(kind, True), (offset, jnp.int32(0)))
        offset = lax.fori_loop(0, jnp.where(more > 0, 64, 0), gather_rest(kind, True), offset)

    subs_f = subs.astype(F32)
    first_row = (group * ROWS).astype(F32)

    def place(taps, base):
        away = subs_f - base
        part = -jnp.floor(away * 0.125)
        index = (away + 8.0 * part).astype(I32)
        turned = jnp.take_along_axis(taps, index, axis=0, mode="promise_in_bounds")
        part = jnp.where(part < 0.0, part + 48.0, part)
        part = jnp.where(part >= 48.0, part - 48.0, part)
        return turned, part

    def pair(part):
        return jnp.concatenate([part, part - 1.0], axis=0).astype(BF16)

    def twice(value):
        return jnp.concatenate([value, value], axis=0).astype(BF16)

    zero = jnp.zeros((16, 128), BF16)

    def prepare(held, at):
        sides = []
        for half in range(2):
            values = packed[at * 2 + half]
            values = jnp.where(lanes + (at * 256 + half * 128) < offset, values, 0.0)
            along_x, along_y, along_z = [jnp.broadcast_to(values[f : f + 1], (8, 128)) for f in range(3)]
            cell_x = jnp.floor(along_x)
            cell_y = jnp.floor(along_y)
            taps_x = kaiser(subs_f - 2.0 - (along_x - cell_x)).astype(BF16).astype(F32)
            taps_y = kaiser(subs_f - 2.0 - (along_y - cell_y))
            taps_z = kaiser(subs_f - along_z)
            turned_x, part_x = place(taps_x, cell_x - 2.0 - first_row)
            turned_y, part_y = place(taps_y, cell_y - 2.0)
            held[half, 0] = turned_x
            held[half, 1] = part_x
            for c in range(2):
                held[half, 2 + c] = taps_z * jnp.broadcast_to(values[3 + c : 4 + c], (8, 128))
            turned_y, part_y = twice(turned_y), pair(part_y)
            sides.append([jnp.where(part_y == group_y, turned_y, zero) for group_y in range(0, NY // 8, 2)] + [zero] * 8)
        for unit in range(2):
            tiles = [jnp.concatenate([side[unit * 16 + at] for side in sides], axis=1) for at in range(16)]
            pltpu.matmul_push_rhs(jnp.concatenate(tiles, axis=0), staging_register=0, mxu_index=unit, transpose=True)

    def stream(held, sums):
        here = []
        for half in range(2):
            part_x = pair(held[half, 1])
            here.append([part_x == group_x for group_x in range(0, ROWS // 8, 2)])
        for plane in range(2 * PLANES):
            z, c = plane // 2, plane % 2
            sides = []
            for half in range(2):
                scaled = twice(held[half, 0] * jnp.broadcast_to(held[half, 2 + c, z : z + 1], (8, 128)))
                sides.append([jnp.where(mask, scaled, zero) for mask in here[half]])
            rows = jnp.concatenate([jnp.concatenate([side[at] for side in sides], axis=1) for at in range(3)], axis=0)
            for unit in range(2):
                pltpu.matmul_acc_lhs(sums[unit][plane], rows, load_staged_rhs=0 if plane == 0 else None)

    def run(*accumulators):
        sums = (accumulators[:12], accumulators[12:])
        prepare(held0, 0)

        def two_chunks(at, carry):
            stream(held0, sums)
            prepare(held1, at * 2 + 1)
            stream(held1, sums)
            prepare(held0, at * 2 + 2)
            return carry

        lax.fori_loop(0, lax.shift_right_logical(offset + 511, 9), two_chunks, 0)
        for unit in range(2):
            pltpu.matmul_acc_lhs(sums[unit][0], jnp.zeros((ROWS, 256), BF16), load_staged_rhs=0)
        lines = flat.reshape(ROWS * PLANES * 6, 128)
        for plane in range(2 * PLANES):
            z, c = plane // 2, plane % 2
            sides = [pltpu.matmul_pop(sums[unit][plane]) for unit in range(2)]
            for y in range(3):
                lines[pl.ds(z * 6 + y * 2 + c, ROWS, stride=36), :] = sides[y // 2][:, (y % 2) * 128 : (y % 2) * 128 + 128]

    pl.run_scoped(run, *[pltpu.ACC(unit)((ROWS, 256), F32) for unit in range(2) for _ in range(12)])
    copies = [pltpu.make_async_copy(flat.at[:, y], out_ref.at[:, :, pl.ds(y * 128, 128)], out_sem.at[y]) for y in range(3)]
    for copy in copies:
        copy.start()
    for copy in copies:
        copy.wait()


def grid_block(everything, group=None):
    vmem = pl.BlockSpec(memory_space=pltpu.VMEM)
    if group is None:
        operands, specs = [everything], [vmem]

        def kernel(all_ref, *refs):
            grid_kernel(lambda: lax.axis_index("grp"), all_ref, *refs)
    else:
        operands, specs = [group, everything], [pl.BlockSpec(memory_space=pltpu.SMEM), vmem]

        def kernel(group_ref, all_ref, *refs):
            grid_kernel(lambda: group_ref[0], all_ref, *refs)

    return pl.pallas_call(
        kernel,
        out_shape=jax.ShapeDtypeStruct((ROWS * PLANES, 2, NY), F32),
        in_specs=specs,
        out_specs=pl.BlockSpec(memory_space=pl.ANY),
        scratch_shapes=[
            pltpu.VMEM((SOURCES, 128), I32),
            pltpu.SMEM((SOURCES, 128), I32),
            pltpu.VMEM((388, 8, 128), F32),
            pltpu.VMEM((2, 4, 8, 128), F32),
            pltpu.VMEM((2, 4, 8, 128), F32),
            pltpu.VMEM((ROWS * PLANES, 3, 2, 128), F32),
            pltpu.SemaphoreType.DMA,
            pltpu.SemaphoreType.DMA((3,)),
        ],
        compiler_params=pltpu.CompilerParams(vmem_limit_bytes=16 * 2**20),
        name="grid_block",
    )(*operands)


def shards(sample_xy, sample_dz, sample_values, block_tile, block_count):
    operands = [block_tile, block_count, sample_xy.reshape(8, 2, 256), sample_dz.reshape(8, 256), sample_values.reshape(8, 2, 256)]
    everything = exchange(*[pltpu.with_memory_space_constraint(operand, pltpu.HBM) for operand in operands])
    block = grid_block(everything.reshape(SOURCES * SEND_ROWS, 128))
    return block.reshape(ROWS, PLANES, 2, NY)


def solution(mesh):
    return jax.shard_map(
        shards,
        mesh=mesh,
        in_specs=(
            P("grp", "slab", None, None, None),
            P("grp", "slab", None, None),
            P("grp", "slab", None, None, None),
            P("grp", "slab", None),
            P("grp", "slab", None),
        ),
        out_specs=P("grp", "slab", None, None),
        check_vma=False,
    )
```

```python
import math

import jax
import jax.numpy as jnp
from jax import lax
from jax.experimental import pallas as pl
from jax.experimental.pallas import tpu as pltpu
from jax.sharding import PartitionSpec as P

NX = 384
NY = 384
PLANES = 6
BLOCKS = 8
GROUPS = 8
ROWS = 48
FIELDS = 5
HALF_ROWS = FIELDS * BLOCKS
TABLE = 2 * HALF_ROWS
SEND_ROWS = TABLE + BLOCKS
SOURCES = 3 * GROUPS
LOW, COUNT, LEFT, WRAP, WRAP_LEFT, ANY_LEFT, HIGH = 0, 8, 32, 56, 80, 104, 112
PIECES = [(0, HALF_ROWS), (HALF_ROWS, SEND_ROWS - HALF_ROWS)]
ORDER = (1, 2, 0)
MESH = pl.DeviceIdType.MESH
BETA = math.pi * math.sqrt(19.45)
F32 = jnp.float32
BF16 = jnp.bfloat16
I32 = jnp.int32


def kaiser_coefficients():
    half_sq = (0.5 * BETA) ** 2
    terms = []
    term = 1.0
    for order in range(1, 32):
        term = term * half_sq / (order * order)
        terms.append(term)
    top = sum(terms)
    return [value / top for value in terms]


COEFF = kaiser_coefficients()


def kaiser(distance):
    third = distance * (1.0 / 3.0)
    inside = jnp.maximum(1.0 - third * third, 0.0)
    square = inside * inside
    fourth = square * square
    chains = []
    for first in range(4):
        picked = COEFF[first::4]
        total = jnp.full_like(inside, picked[-1])
        for value in picked[-2::-1]:
            total = total * fourth + value
        chains.append(total)
    low = chains[0] + chains[1] * inside
    high = chains[2] + chains[3] * inside
    return (low + high * square) * inside


def sort_blocks(tile_ref, count_ref, xy_ref, dz_ref, val_ref, out_ref, fields):
    lanes = lax.broadcasted_iota(I32, (BLOCKS, 256), 1)
    subs = lax.broadcasted_iota(I32, (BLOCKS, 256), 0)
    counts = jnp.zeros((BLOCKS, 256), I32)
    tiles = jnp.zeros((BLOCKS, 256), I32)
    for b in range(BLOCKS):
        counts = jnp.where(subs == b, count_ref[0, 0, b], counts)
        tiles = jnp.where(subs == b, tile_ref[0, 0, b], tiles)
    along_x = xy_ref[:, 0, :]
    cell = jnp.floor(along_x)
    shifted = cell + 3.0
    shifted = jnp.where(shifted >= NX, shifted - NX, shifted)
    shifted = jnp.where(lanes < counts, shifted, 400.0)
    fields[0:8] = along_x
    fields[8:16] = xy_ref[:, 1, :]
    fields[16:24] = dz_ref[...] + tiles.astype(F32)
    fields[24:32] = val_ref[:, 0, :]
    fields[32:40] = val_ref[:, 1, :]

    def below(bound):
        return jnp.sum(jnp.where(shifted < bound, 1.0, 0.0), axis=1, keepdims=True)

    column = lanes[:, 0:128]
    tile_f = tiles[:, 0:128].astype(F32)
    kinds = [jnp.ones((BLOCKS, 128), F32), jnp.where(tile_f > 2.5, 1.0, 0.0), jnp.where(tile_f < 1.5, 1.0, 0.0)]
    table = jnp.zeros((BLOCKS, 128), F32)
    for group in range(GROUPS):
        start = below(float(ROWS * group))
        count = below(float(ROWS * group + ROWS + 5)) - start
        first = jnp.minimum(count, 128.0)
        start = jnp.minimum(start, 255.0)
        high = jnp.where(start > 127.5, 1.0, 0.0)
        table = jnp.where(column == LOW + group, start - 128.0 * high, table)
        table = jnp.where(column == HIGH + group, high * HALF_ROWS, table)
        for kind in range(3):
            table = jnp.where(column == COUNT + 8 * kind + group, first * kinds[kind], table)
            table = jnp.where(column == LEFT + 8 * kind + group, (count - first) * kinds[kind], table)
    count = below(5.0)
    first = jnp.minimum(count, 128.0)
    for kind in range(3):
        table = jnp.where(column == WRAP + kind, first * kinds[kind], table)
        table = jnp.where(column == WRAP + 3 + kind, (count - first) * kinds[kind], table)
    table = table.T
    pieces = [table[at : at + 8] for at in range(0, WRAP, 8)]
    pieces += [jnp.broadcast_to(table[WRAP + at : WRAP + at + 1], (8, 8)) for at in range(6)]
    left = pieces[4] + pieces[10]
    pieces.append(jnp.broadcast_to(jnp.sum(left, axis=1, keepdims=True), (8, 8)))
    pieces.append(table[HIGH : HIGH + 8])
    out_ref[TABLE : TABLE + BLOCKS, :] = jnp.concatenate(pieces + [jnp.zeros((8, 128 - 8 * len(pieces)), F32)], axis=1)
    key = shifted * 256.0 + lanes.astype(F32)
    key_t = key.T
    place = lax.broadcasted_iota(I32, (256, 256), 0).astype(F32)
    for b in range(BLOCKS):
        before = key_t[:, b : b + 1] < key[b : b + 1, :]
        rank = jnp.sum(jnp.where(before, 1.0, 0.0), axis=0, keepdims=True)
        pick = jnp.where(place == rank, 1.0, 0.0).astype(BF16)
        rows = jnp.concatenate([fields[f * 8 + b : f * 8 + b + 1, :] for f in range(5)] + [jnp.zeros((3, 256), F32)], axis=0)
        top = rows.astype(BF16)
        rest = rows - top.astype(F32)
        mid = rest.astype(BF16)
        low = (rest - mid.astype(F32)).astype(BF16)
        parts = jnp.concatenate([top.astype(F32), mid.astype(F32), low.astype(F32)], axis=0).astype(BF16)
        moved = lax.dot_general(parts, pick, (((1,), (1,)), ((), ())), preferred_element_type=F32)
        ordered = (moved[0:8] + moved[8:16]) + moved[16:24]
        for f in range(FIELDS):
            for half in range(2):
                row = half * HALF_ROWS + f * 8 + b
                out_ref[row : row + 1, :] = ordered[f : f + 1, half * 128 : half * 128 + 128]


def exchange_kernel(
    tile_in, count_in, xy_in, dz_in, val_in, out_ref, tile_ref, count_ref, xy_ref, dz_ref, val_ref, fields, own_ref, in_sem, send_sem, recv_sem
):
    loads = [
        pltpu.make_async_copy(source, target, in_sem.at[at])
        for at, (source, target) in enumerate(
            [(xy_in, xy_ref), (tile_in, tile_ref), (count_in, count_ref), (dz_in, dz_ref), (val_in, val_ref)]
        )
    ]
    for load in loads:
        load.start()
    grp = lax.axis_index("grp")
    slab = lax.axis_index("slab")
    far = lax.rem(grp + 4, 8)
    half = (grp // 4) * 4
    spot = grp - half
    peers = [half + lax.rem(spot + step, 4) for step in (2, 1, 3)]
    far_half = 4 - half
    core = lax.rem(slab, 2)
    outer = lax.rem(slab + 31 - 30 * core, 32)
    inner = lax.rem(slab + 1 + 30 * core, 32)
    beside = [((grp, outer), 2 - core), ((grp, inner), 1 + core)]
    around = [(far, slab)] + [(peer, slab) for peer in peers] + [(grp, outer), (grp, inner)]

    barrier = pltpu.get_barrier_semaphore()
    for device in around:
        pl.semaphore_signal(barrier, inc=1, device_id=device, device_id_type=MESH)
    for load in loads:
        load.wait()
    sort_blocks(tile_ref, count_ref, xy_ref, dz_ref, val_ref, own_ref, fields)
    pl.semaphore_wait(barrier, len(around))

    sends = []

    def rows_of(ref, rows):
        return ref if rows is None else ref.at[pl.ds(rows[0], rows[1])]

    def send(source, kind, owner, item, device, rows=None):
        copy = pltpu.make_async_remote_copy(
            src_ref=rows_of(source, rows),
            dst_ref=rows_of(out_ref.at[kind, owner], rows),
            send_sem=send_sem.at[len(sends)],
            recv_sem=recv_sem.at[kind, item],
            device_id=device,
            device_id_type=MESH,
        )
        copy.start()
        sends.append(copy)

    def arrive(kind, owner, item, rows=None):
        pltpu.make_async_remote_copy(
            src_ref=rows_of(own_ref, rows),
            dst_ref=rows_of(out_ref.at[kind, owner], rows),
            send_sem=send_sem.at[0],
            recv_sem=recv_sem.at[kind, item],
            device_id=(grp, slab),
            device_id_type=MESH,
        ).wait_recv()

    pieces = PIECES
    count = len(pieces)
    for at, rows in enumerate(pieces):
        send(own_ref, 0, grp, 4 + at, (far, slab), rows)
    for at, peer in enumerate(peers):
        send(own_ref, 0, grp, 1 + at, (peer, slab))
    for device, kind in beside:
        send(own_ref, kind, grp, 0, device)
    out_ref[0, grp] = own_ref[...]
    back = [half + lax.rem(spot + step, 4) for step in (2, 3, 1)]
    for at in ORDER:
        arrive(0, back[at], 1 + at)
        for device, kind in beside:
            send(out_ref.at[0, back[at]], kind, back[at], 1 + at, device)
    for piece, rows in enumerate(pieces):
        arrive(0, far, 4 + piece, rows)
        for at, peer in enumerate(peers):
            send(out_ref.at[0, far], 0, far, 4 + count + count * at + piece, (peer, slab), rows)
        for device, kind in beside:
            send(out_ref.at[0, far], kind, far, 4 + piece, device, rows)
    for piece, rows in enumerate(pieces):
        for at in ORDER:
            owner = back[at] - half + far_half
            arrive(0, owner, 4 + count + count * at + piece, rows)
            for device, kind in beside:
                send(out_ref.at[0, owner], kind, owner, 4 + count + count * at + piece, device, rows)
    for kind in (1, 2):
        arrive(kind, grp, 0)
        for at in range(3):
            arrive(kind, back[at], 1 + at)
        for piece, rows in enumerate(pieces):
            arrive(kind, far, 4 + piece, rows)
            for at in range(3):
                arrive(kind, back[at] - half + far_half, 4 + count + count * at + piece, rows)
    for copy in sends:
        copy.wait_send()


def exchange(tile, count, xy, dz, val):
    vmem = pl.BlockSpec(memory_space=pltpu.VMEM)
    hbm = pl.BlockSpec(memory_space=pltpu.HBM)
    return pl.pallas_call(
        exchange_kernel,
        out_shape=jax.ShapeDtypeStruct((3, GROUPS, SEND_ROWS, 128), F32),
        in_specs=[hbm] * 5,
        out_specs=vmem,
        scratch_shapes=[
            pltpu.SMEM((1, 1, 8), I32),
            pltpu.SMEM((1, 1, 8), I32),
            pltpu.VMEM((BLOCKS, 2, 256), F32),
            pltpu.VMEM((BLOCKS, 256), F32),
            pltpu.VMEM((BLOCKS, 2, 256), F32),
            pltpu.VMEM((HALF_ROWS, 256), F32),
            pltpu.VMEM((SEND_ROWS, 128), F32),
            pltpu.SemaphoreType.DMA((5,)),
            pltpu.SemaphoreType.DMA((11 + 12 * len(PIECES),)),
            pltpu.SemaphoreType.DMA((3, 4 + 4 * len(PIECES))),
        ],
        compiler_params=pltpu.CompilerParams(collective_id=0, has_side_effects=True, vmem_limit_bytes=8 * 2**20),
        name="exchange",
    )(tile, count, xy, dz, val)


def grid_kernel(read_group, all_ref, out_ref, table_v, table, packed, held0, held1, flat, sem, out_sem):
    group = read_group()
    for source in range(SOURCES):
        table_v[source : source + 1, :] = all_ref[pl.ds(source * SEND_ROWS + TABLE + group, 1), :].astype(I32)
    copy = pltpu.make_async_copy(table_v, table, sem)
    copy.start()
    lanes = lax.broadcasted_iota(I32, (8, 128), 1)
    lanes_f = lanes[:FIELDS]
    subs = lax.broadcasted_iota(I32, (8, 128), 0)
    copy.wait()

    def append(kind, source, b, low, rows, count, offset):
        first = source * SEND_ROWS + b
        values = all_ref[pl.ds(first + rows, FIELDS, stride=8), :]
        after = all_ref[pl.ds(first + HALF_ROWS, FIELDS, stride=8), :]
        values = jnp.where(lanes_f >= low, values, after)
        if kind > 0:
            values = values + jnp.where(subs[:FIELDS] == 2, (0.0, -6.0, 6.0)[kind], 0.0)
        at = lax.bitwise_and(offset, 127)
        rolled = pltpu.roll(values, lax.bitwise_and(at - low, 127), 1)
        slot = lax.shift_right_logical(offset, 7)
        pltpu.store(packed.at[slot, 0:FIELDS], rolled, mask=lanes_f >= at)
        packed[slot + 1, 0:FIELDS] = rolled
        return offset + count

    def span(wrap, source, b):
        return (jnp.int32(0), jnp.int32(0)) if wrap else (table[source, LOW + b], table[source, HIGH + b])

    def gather(kind, wrap):
        def body(at, carry):
            offset, more = carry
            source = kind * GROUPS + at
            for b in range(BLOCKS):
                low, rows = span(wrap, source, b)
                offset = append(kind, source, b, low, rows, table[source, (WRAP if wrap else COUNT) + 8 * kind + b], offset)
            return offset, more + table[source, ANY_LEFT]

        return body

    def gather_rest(kind, wrap):
        def body(at, offset):
            source = kind * GROUPS + lax.shift_right_logical(at, 3)
            b = lax.bitwise_and(at, 7)
            low = span(wrap, source, b)[0]
            left = table[source, (WRAP_LEFT if wrap else LEFT) + 8 * kind + b]
            return lax.cond(left > 0, lambda o: append(kind, source, b, low, HALF_ROWS, left, o), lambda o: o, offset)

        return body

    offset = jnp.int32(0)
    for kind in range(3):
        more = jnp.int32(0)
        for at in range(GROUPS):
            offset, more = gather(kind, False)(at, (offset, more))
        offset = lax.fori_loop(0, jnp.where(more > 0, 64, 0), gather_rest(kind, False), offset)
    for kind in range(3):
        steps = jnp.where(group == GROUPS - 1, GROUPS, 0)
        offset, more = lax.fori_loop(0, steps, gather(kind, True), (offset, jnp.int32(0)))
        offset = lax.fori_loop(0, jnp.where(more > 0, 64, 0), gather_rest(kind, True), offset)

    subs_f = subs.astype(F32)
    first_row = (group * ROWS).astype(F32)

    def place(taps, base):
        away = subs_f - base
        part = -jnp.floor(away * 0.125)
        index = (away + 8.0 * part).astype(I32)
        turned = jnp.take_along_axis(taps, index, axis=0, mode="promise_in_bounds")
        part = jnp.where(part < 0.0, part + 48.0, part)
        part = jnp.where(part >= 48.0, part - 48.0, part)
        return turned, part

    def pair(part):
        return jnp.concatenate([part, part - 1.0], axis=0).astype(BF16)

    def twice(value):
        return jnp.concatenate([value, value], axis=0).astype(BF16)

    zero = jnp.zeros((16, 128), BF16)

    def prepare(held, at):
        sides = []
        for half in range(2):
            values = packed[at * 2 + half]
            values = jnp.where(lanes + (at * 256 + half * 128) < offset, values, 0.0)
            along_x, along_y, along_z = [jnp.broadcast_to(values[f : f + 1], (8, 128)) for f in range(3)]
            cell_x = jnp.floor(along_x)
            cell_y = jnp.floor(along_y)
            taps_x = kaiser(subs_f - 2.0 - (along_x - cell_x)).astype(BF16).astype(F32)
            taps_y = kaiser(subs_f - 2.0 - (along_y - cell_y))
            taps_z = kaiser(subs_f - along_z)
            turned_x, part_x = place(taps_x, cell_x - 2.0 - first_row)
            turned_y, part_y = place(taps_y, cell_y - 2.0)
            held[half, 0] = turned_x
            held[half, 1] = part_x
            for c in range(2):
                held[half, 2 + c] = taps_z * jnp.broadcast_to(values[3 + c : 4 + c], (8, 128))
            turned_y, part_y = twice(turned_y), pair(part_y)
            sides.append([jnp.where(part_y == group_y, turned_y, zero) for group_y in range(0, NY // 8, 2)] + [zero] * 8)
        for unit in range(2):
            tiles = [jnp.concatenate([side[unit * 16 + at] for side in sides], axis=1) for at in range(16)]
            pltpu.matmul_push_rhs(jnp.concatenate(tiles, axis=0), staging_register=0, mxu_index=unit, transpose=True)

    def stream(held, sums):
        here = []
        for half in range(2):
            part_x = pair(held[half, 1])
            here.append([part_x == group_x for group_x in range(0, ROWS // 8, 2)])
        for plane in range(2 * PLANES):
            z, c = plane // 2, plane % 2
            sides = []
            for half in range(2):
                scaled = twice(held[half, 0] * jnp.broadcast_to(held[half, 2 + c, z : z + 1], (8, 128)))
                sides.append([jnp.where(mask, scaled, zero) for mask in here[half]])
            rows = jnp.concatenate([jnp.concatenate([side[at] for side in sides], axis=1) for at in range(3)], axis=0)
            for unit in range(2):
                pltpu.matmul_acc_lhs(sums[unit][plane], rows, load_staged_rhs=0 if plane == 0 else None)

    def run(*accumulators):
        sums = (accumulators[:12], accumulators[12:])
        prepare(held0, 0)

        def two_chunks(at, carry):
            stream(held0, sums)
            prepare(held1, at * 2 + 1)
            stream(held1, sums)
            prepare(held0, at * 2 + 2)
            return carry

        chunks = lax.shift_right_logical(offset + 255, 8)
        lax.fori_loop(0, lax.shift_right_logical(chunks, 1), two_chunks, 0)

        @pl.when(lax.bitwise_and(chunks, 1) == 1)
        def _():
            stream(held0, sums)

        @pl.when(lax.bitwise_and(chunks, 1) == 0)
        def _():
            for unit in range(2):
                pltpu.matmul_acc_lhs(sums[unit][0], jnp.zeros((ROWS, 256), BF16), load_staged_rhs=0)

        lines = flat.reshape(ROWS * PLANES * 6, 128)
        for plane in range(2 * PLANES):
            z, c = plane // 2, plane % 2
            sides = [pltpu.matmul_pop(sums[unit][plane]) for unit in range(2)]
            for y in range(3):
                lines[pl.ds(z * 6 + y * 2 + c, ROWS, stride=36), :] = sides[y // 2][:, (y % 2) * 128 : (y % 2) * 128 + 128]

    pl.run_scoped(run, *[pltpu.ACC(unit)((ROWS, 256), F32) for unit in range(2) for _ in range(12)])
    copies = [pltpu.make_async_copy(flat.at[:, y], out_ref.at[:, :, pl.ds(y * 128, 128)], out_sem.at[y]) for y in range(3)]
    for copy in copies:
        copy.start()
    for copy in copies:
        copy.wait()


def grid_block(everything, group=None):
    vmem = pl.BlockSpec(memory_space=pltpu.VMEM)
    if group is None:
        operands, specs = [everything], [vmem]

        def kernel(all_ref, *refs):
            grid_kernel(lambda: lax.axis_index("grp"), all_ref, *refs)
    else:
        operands, specs = [group, everything], [pl.BlockSpec(memory_space=pltpu.SMEM), vmem]

        def kernel(group_ref, all_ref, *refs):
            grid_kernel(lambda: group_ref[0], all_ref, *refs)

    return pl.pallas_call(
        kernel,
        out_shape=jax.ShapeDtypeStruct((ROWS * PLANES, 2, NY), F32),
        in_specs=specs,
        out_specs=pl.BlockSpec(memory_space=pl.ANY),
        scratch_shapes=[
            pltpu.VMEM((SOURCES, 128), I32),
            pltpu.SMEM((SOURCES, 128), I32),
            pltpu.VMEM((388, 8, 128), F32),
            pltpu.VMEM((2, 4, 8, 128), F32),
            pltpu.VMEM((2, 4, 8, 128), F32),
            pltpu.VMEM((ROWS * PLANES, 3, 2, 128), F32),
            pltpu.SemaphoreType.DMA,
            pltpu.SemaphoreType.DMA((3,)),
        ],
        compiler_params=pltpu.CompilerParams(vmem_limit_bytes=16 * 2**20),
        name="grid_block",
    )(*operands)


def shards(sample_xy, sample_dz, sample_values, block_tile, block_count):
    operands = [block_tile, block_count, sample_xy.reshape(8, 2, 256), sample_dz.reshape(8, 256), sample_values.reshape(8, 2, 256)]
    everything = exchange(*[pltpu.with_memory_space_constraint(operand, pltpu.HBM) for operand in operands])
    block = grid_block(everything.reshape(SOURCES * SEND_ROWS, 128))
    return block.reshape(ROWS, PLANES, 2, NY)


def solution(mesh):
    return jax.shard_map(
        shards,
        mesh=mesh,
        in_specs=(
            P("grp", "slab", None, None, None),
            P("grp", "slab", None, None),
            P("grp", "slab", None, None, None),
            P("grp", "slab", None),
            P("grp", "slab", None),
        ),
        out_specs=P("grp", "slab", None, None),
        check_vma=False,
    )
```

```python
import math

import jax
import jax.numpy as jnp
from jax import lax
from jax.experimental import pallas as pl
from jax.experimental.pallas import tpu as pltpu
from jax.sharding import PartitionSpec as P

NX = 384
NY = 384
PLANES = 6
BLOCKS = 8
GROUPS = 8
ROWS = 48
FIELDS = 5
HALF_ROWS = FIELDS * BLOCKS
TABLE = 2 * HALF_ROWS
SEND_ROWS = TABLE + BLOCKS
SOURCES = 3 * GROUPS
LOW, COUNT, LEFT, WRAP, WRAP_LEFT, ANY_LEFT, HIGH = 0, 8, 32, 56, 80, 104, 112
PIECES = [(0, HALF_ROWS), (HALF_ROWS, SEND_ROWS - HALF_ROWS)]
ORDER = (1, 2, 0)
MESH = pl.DeviceIdType.MESH
BETA = math.pi * math.sqrt(19.45)
F32 = jnp.float32
BF16 = jnp.bfloat16
I32 = jnp.int32


def kaiser_coefficients():
    half_sq = (0.5 * BETA) ** 2
    terms = []
    term = 1.0
    for order in range(1, 32):
        term = term * half_sq / (order * order)
        terms.append(term)
    top = sum(terms)
    return [value / top for value in terms]


COEFF = kaiser_coefficients()


def kaiser(distance):
    third = distance * (1.0 / 3.0)
    inside = jnp.maximum(1.0 - third * third, 0.0)
    square = inside * inside
    fourth = square * square
    chains = []
    for first in range(4):
        picked = COEFF[first::4]
        total = jnp.full_like(inside, picked[-1])
        for value in picked[-2::-1]:
            total = total * fourth + value
        chains.append(total)
    low = chains[0] + chains[1] * inside
    high = chains[2] + chains[3] * inside
    return (low + high * square) * inside


def sort_blocks(tile_ref, count_ref, xy_ref, dz_ref, val_ref, out_ref, fields):
    lanes = lax.broadcasted_iota(I32, (BLOCKS, 256), 1)
    subs = lax.broadcasted_iota(I32, (BLOCKS, 256), 0)
    counts = jnp.zeros((BLOCKS, 256), I32)
    tiles = jnp.zeros((BLOCKS, 256), I32)
    for b in range(BLOCKS):
        counts = jnp.where(subs == b, count_ref[0, 0, b], counts)
        tiles = jnp.where(subs == b, tile_ref[0, 0, b], tiles)
    along_x = xy_ref[:, 0, :]
    cell = jnp.floor(along_x)
    shifted = cell + 3.0
    shifted = jnp.where(shifted >= NX, shifted - NX, shifted)
    shifted = jnp.where(lanes < counts, shifted, 400.0)
    fields[0:8] = along_x
    fields[8:16] = xy_ref[:, 1, :]
    fields[16:24] = dz_ref[...] + tiles.astype(F32)
    fields[24:32] = val_ref[:, 0, :]
    fields[32:40] = val_ref[:, 1, :]

    def below(bound):
        return jnp.sum(jnp.where(shifted < bound, 1.0, 0.0), axis=1, keepdims=True)

    column = lanes[:, 0:128]
    tile_f = tiles[:, 0:128].astype(F32)
    kinds = [jnp.ones((BLOCKS, 128), F32), jnp.where(tile_f > 2.5, 1.0, 0.0), jnp.where(tile_f < 1.5, 1.0, 0.0)]
    table = jnp.zeros((BLOCKS, 128), F32)
    for group in range(GROUPS):
        start = below(float(ROWS * group))
        count = below(float(ROWS * group + ROWS + 5)) - start
        first = jnp.minimum(count, 128.0)
        start = jnp.minimum(start, 255.0)
        high = jnp.where(start > 127.5, 1.0, 0.0)
        table = jnp.where(column == LOW + group, start - 128.0 * high, table)
        table = jnp.where(column == HIGH + group, high * HALF_ROWS, table)
        for kind in range(3):
            table = jnp.where(column == COUNT + 8 * kind + group, first * kinds[kind], table)
            table = jnp.where(column == LEFT + 8 * kind + group, (count - first) * kinds[kind], table)
    count = below(5.0)
    first = jnp.minimum(count, 128.0)
    for kind in range(3):
        table = jnp.where(column == WRAP + kind, first * kinds[kind], table)
        table = jnp.where(column == WRAP + 3 + kind, (count - first) * kinds[kind], table)
    table = table.T
    pieces = [table[at : at + 8] for at in range(0, WRAP, 8)]
    pieces += [jnp.broadcast_to(table[WRAP + at : WRAP + at + 1], (8, 8)) for at in range(6)]
    left = pieces[4] + pieces[10]
    pieces.append(jnp.broadcast_to(jnp.sum(left, axis=1, keepdims=True), (8, 8)))
    pieces.append(table[HIGH : HIGH + 8])
    out_ref[TABLE : TABLE + BLOCKS, :] = jnp.concatenate(pieces + [jnp.zeros((8, 128 - 8 * len(pieces)), F32)], axis=1)
    key = shifted * 256.0 + lanes.astype(F32)
    key_t = key.T
    place = lax.broadcasted_iota(I32, (256, 256), 0).astype(F32)
    for b in range(BLOCKS):
        before = key_t[:, b : b + 1] < key[b : b + 1, :]
        rank = jnp.sum(jnp.where(before, 1.0, 0.0), axis=0, keepdims=True)
        pick = jnp.where(place == rank, 1.0, 0.0).astype(BF16)
        rows = jnp.concatenate([fields[f * 8 + b : f * 8 + b + 1, :] for f in range(5)] + [jnp.zeros((3, 256), F32)], axis=0)
        top = rows.astype(BF16)
        rest = rows - top.astype(F32)
        mid = rest.astype(BF16)
        low = (rest - mid.astype(F32)).astype(BF16)
        parts = jnp.concatenate([top.astype(F32), mid.astype(F32), low.astype(F32)], axis=0).astype(BF16)
        moved = lax.dot_general(parts, pick, (((1,), (1,)), ((), ())), preferred_element_type=F32)
        ordered = (moved[0:8] + moved[8:16]) + moved[16:24]
        for f in range(FIELDS):
            for half in range(2):
                row = half * HALF_ROWS + f * 8 + b
                out_ref[row : row + 1, :] = ordered[f : f + 1, half * 128 : half * 128 + 128]


def exchange_kernel(
    tile_in, count_in, xy_in, dz_in, val_in, out_ref, tile_ref, count_ref, xy_ref, dz_ref, val_ref, fields, own_ref, in_sem, send_sem, recv_sem
):
    loads = [
        pltpu.make_async_copy(source, target, in_sem.at[at])
        for at, (source, target) in enumerate(
            [(xy_in, xy_ref), (tile_in, tile_ref), (count_in, count_ref), (dz_in, dz_ref), (val_in, val_ref)]
        )
    ]
    for load in loads:
        load.start()
    grp = lax.axis_index("grp")
    slab = lax.axis_index("slab")
    far = lax.rem(grp + 4, 8)
    half = (grp // 4) * 4
    spot = grp - half
    peers = [half + lax.rem(spot + step, 4) for step in (2, 1, 3)]
    far_half = 4 - half
    core = lax.rem(slab, 2)
    outer = lax.rem(slab + 31 - 30 * core, 32)
    inner = lax.rem(slab + 1 + 30 * core, 32)
    beside = [((grp, outer), 2 - core), ((grp, inner), 1 + core)]
    around = [(far, slab)] + [(peer, slab) for peer in peers] + [(grp, outer), (grp, inner)]

    barrier = pltpu.get_barrier_semaphore()
    for device in around:
        pl.semaphore_signal(barrier, inc=1, device_id=device, device_id_type=MESH)
    for load in loads:
        load.wait()
    sort_blocks(tile_ref, count_ref, xy_ref, dz_ref, val_ref, own_ref, fields)
    pl.semaphore_wait(barrier, len(around))

    sends = []

    def rows_of(ref, rows):
        return ref if rows is None else ref.at[pl.ds(rows[0], rows[1])]

    def send(source, kind, owner, item, device, rows=None):
        copy = pltpu.make_async_remote_copy(
            src_ref=rows_of(source, rows),
            dst_ref=rows_of(out_ref.at[kind, owner], rows),
            send_sem=send_sem.at[len(sends)],
            recv_sem=recv_sem.at[kind, item],
            device_id=device,
            device_id_type=MESH,
        )
        copy.start()
        sends.append(copy)

    def arrive(kind, owner, item, rows=None):
        pltpu.make_async_remote_copy(
            src_ref=rows_of(own_ref, rows),
            dst_ref=rows_of(out_ref.at[kind, owner], rows),
            send_sem=send_sem.at[0],
            recv_sem=recv_sem.at[kind, item],
            device_id=(grp, slab),
            device_id_type=MESH,
        ).wait_recv()

    pieces = PIECES
    count = len(pieces)
    for at, rows in enumerate(pieces):
        send(own_ref, 0, grp, 4 + at, (far, slab), rows)
    for at, peer in enumerate(peers):
        send(own_ref, 0, grp, 1 + at, (peer, slab))
    for device, kind in beside:
        send(own_ref, kind, grp, 0, device)
    out_ref[0, grp] = own_ref[...]
    back = [half + lax.rem(spot + step, 4) for step in (2, 3, 1)]
    for at in ORDER:
        arrive(0, back[at], 1 + at)
        for device, kind in beside:
            send(out_ref.at[0, back[at]], kind, back[at], 1 + at, device)
    for piece, rows in enumerate(pieces):
        arrive(0, far, 4 + piece, rows)
        for at, peer in enumerate(peers):
            send(out_ref.at[0, far], 0, far, 4 + count + count * at + piece, (peer, slab), rows)
        for device, kind in beside:
            send(out_ref.at[0, far], kind, far, 4 + piece, device, rows)
    for piece, rows in enumerate(pieces):
        for at in ORDER:
            owner = back[at] - half + far_half
            arrive(0, owner, 4 + count + count * at + piece, rows)
            for device, kind in beside:
                send(out_ref.at[0, owner], kind, owner, 4 + count + count * at + piece, device, rows)
    for kind in (1, 2):
        arrive(kind, grp, 0)
        for at in range(3):
            arrive(kind, back[at], 1 + at)
        for piece, rows in enumerate(pieces):
            arrive(kind, far, 4 + piece, rows)
            for at in range(3):
                arrive(kind, back[at] - half + far_half, 4 + count + count * at + piece, rows)
    for copy in sends:
        copy.wait_send()


def exchange(tile, count, xy, dz, val):
    vmem = pl.BlockSpec(memory_space=pltpu.VMEM)
    hbm = pl.BlockSpec(memory_space=pltpu.HBM)
    return pl.pallas_call(
        exchange_kernel,
        out_shape=jax.ShapeDtypeStruct((3, GROUPS, SEND_ROWS, 128), F32),
        in_specs=[hbm] * 5,
        out_specs=vmem,
        scratch_shapes=[
            pltpu.SMEM((1, 1, 8), I32),
            pltpu.SMEM((1, 1, 8), I32),
            pltpu.VMEM((BLOCKS, 2, 256), F32),
            pltpu.VMEM((BLOCKS, 256), F32),
            pltpu.VMEM((BLOCKS, 2, 256), F32),
            pltpu.VMEM((HALF_ROWS, 256), F32),
            pltpu.VMEM((SEND_ROWS, 128), F32),
            pltpu.SemaphoreType.DMA((5,)),
            pltpu.SemaphoreType.DMA((11 + 12 * len(PIECES),)),
            pltpu.SemaphoreType.DMA((3, 4 + 4 * len(PIECES))),
        ],
        compiler_params=pltpu.CompilerParams(collective_id=0, has_side_effects=True, vmem_limit_bytes=8 * 2**20),
        name="exchange",
    )(tile, count, xy, dz, val)


def grid_kernel(read_group, all_ref, out_ref, table_v, table, packed, held0, held1, flat, sem, out_sem):
    group = read_group()
    for source in range(SOURCES):
        table_v[source : source + 1, :] = all_ref[pl.ds(source * SEND_ROWS + TABLE + group, 1), :].astype(I32)
    copy = pltpu.make_async_copy(table_v, table, sem)
    copy.start()
    lanes = lax.broadcasted_iota(I32, (8, 128), 1)
    lanes_f = lanes[:FIELDS]
    subs = lax.broadcasted_iota(I32, (8, 128), 0)
    copy.wait()

    def append(kind, source, b, low, rows, count, offset):
        first = source * SEND_ROWS + b
        values = all_ref[pl.ds(first + rows, FIELDS, stride=8), :]
        after = all_ref[pl.ds(first + HALF_ROWS, FIELDS, stride=8), :]
        values = jnp.where(lanes_f >= low, values, after)
        if kind > 0:
            values = values + jnp.where(subs[:FIELDS] == 2, (0.0, -6.0, 6.0)[kind], 0.0)
        at = lax.bitwise_and(offset, 127)
        rolled = pltpu.roll(values, lax.bitwise_and(at - low, 127), 1)
        slot = lax.shift_right_logical(offset, 7)
        pltpu.store(packed.at[slot, 0:FIELDS], rolled, mask=lanes_f >= at)
        packed[slot + 1, 0:FIELDS] = rolled
        return offset + count

    def span(wrap, source, b):
        return (jnp.int32(0), jnp.int32(0)) if wrap else (table[source, LOW + b], table[source, HIGH + b])

    def gather(kind, wrap):
        def body(at, carry):
            offset, more = carry
            source = kind * GROUPS + at
            for b in range(BLOCKS):
                low, rows = span(wrap, source, b)
                offset = append(kind, source, b, low, rows, table[source, (WRAP if wrap else COUNT) + 8 * kind + b], offset)
            return offset, more + table[source, ANY_LEFT]

        return body

    def gather_rest(kind, wrap):
        def body(at, offset):
            source = kind * GROUPS + lax.shift_right_logical(at, 3)
            b = lax.bitwise_and(at, 7)
            low = span(wrap, source, b)[0]
            left = table[source, (WRAP_LEFT if wrap else LEFT) + 8 * kind + b]
            return lax.cond(left > 0, lambda o: append(kind, source, b, low, HALF_ROWS, left, o), lambda o: o, offset)

        return body

    def gather_kind(kind, offset):
        more = jnp.int32(0)
        for at in range(GROUPS):
            offset, more = gather(kind, False)(at, (offset, more))
        return offset, more

    def gather_others(offset, left):
        for kind in range(3):
            offset = lax.fori_loop(0, jnp.where(left[kind] > 0, 64, 0), gather_rest(kind, False), offset)
        for kind in range(3):
            steps = jnp.where(group == GROUPS - 1, GROUPS, 0)
            offset, more = lax.fori_loop(0, steps, gather(kind, True), (offset, jnp.int32(0)))
            offset = lax.fori_loop(0, jnp.where(more > 0, 64, 0), gather_rest(kind, True), offset)
        return offset

    subs_f = subs.astype(F32)
    first_row = (group * ROWS).astype(F32)

    def place(taps, base):
        away = subs_f - base
        part = -jnp.floor(away * 0.125)
        index = (away + 8.0 * part).astype(I32)
        turned = jnp.take_along_axis(taps, index, axis=0, mode="promise_in_bounds")
        part = jnp.where(part < 0.0, part + 48.0, part)
        part = jnp.where(part >= 48.0, part - 48.0, part)
        return turned, part

    def pair(part):
        return jnp.concatenate([part, part - 1.0], axis=0).astype(BF16)

    def twice(value):
        return jnp.concatenate([value, value], axis=0).astype(BF16)

    zero = jnp.zeros((16, 128), BF16)

    def prepare(held, at, offset):
        sides = []
        for half in range(2):
            values = packed[at * 2 + half]
            values = jnp.where(lanes + (at * 256 + half * 128) < offset, values, 0.0)
            along_x, along_y, along_z = [jnp.broadcast_to(values[f : f + 1], (8, 128)) for f in range(3)]
            cell_x = jnp.floor(along_x)
            cell_y = jnp.floor(along_y)
            taps_x = kaiser(subs_f - 2.0 - (along_x - cell_x)).astype(BF16).astype(F32)
            taps_y = kaiser(subs_f - 2.0 - (along_y - cell_y))
            taps_z = kaiser(subs_f - along_z)
            turned_x, part_x = place(taps_x, cell_x - 2.0 - first_row)
            turned_y, part_y = place(taps_y, cell_y - 2.0)
            held[half, 0] = turned_x
            held[half, 1] = part_x
            for c in range(2):
                held[half, 2 + c] = taps_z * jnp.broadcast_to(values[3 + c : 4 + c], (8, 128))
            turned_y, part_y = twice(turned_y), pair(part_y)
            sides.append([jnp.where(part_y == group_y, turned_y, zero) for group_y in range(0, NY // 8, 2)] + [zero] * 8)
        for unit in range(2):
            tiles = [jnp.concatenate([side[unit * 16 + at] for side in sides], axis=1) for at in range(16)]
            pltpu.matmul_push_rhs(jnp.concatenate(tiles, axis=0), staging_register=0, mxu_index=unit, transpose=True)

    def stream(held, sums):
        here = []
        for half in range(2):
            part_x = pair(held[half, 1])
            here.append([part_x == group_x for group_x in range(0, ROWS // 8, 2)])
        for plane in range(2 * PLANES):
            z, c = plane // 2, plane % 2
            sides = []
            for half in range(2):
                scaled = twice(held[half, 0] * jnp.broadcast_to(held[half, 2 + c, z : z + 1], (8, 128)))
                sides.append([jnp.where(mask, scaled, zero) for mask in here[half]])
            rows = jnp.concatenate([jnp.concatenate([side[at] for side in sides], axis=1) for at in range(3)], axis=0)
            for unit in range(2):
                pltpu.matmul_acc_lhs(sums[unit][plane], rows, load_staged_rhs=0 if plane == 0 else None)

    def run(*accumulators):
        sums = (accumulators[:12], accumulators[12:])
        own, left_own = gather_kind(0, jnp.int32(0))

        def gather_beside(offset):
            offset, left_below = gather_kind(1, offset)
            offset, left_above = gather_kind(2, offset)
            return offset, left_below, left_above

        def with_chunks(offset):
            prepare(held0, 0, offset)
            prepare_next = offset
            stream(held0, sums)
            offset, left_below = gather_kind(1, offset)
            prepare(held1, 1, prepare_next)
            stream(held1, sums)
            offset, left_above = gather_kind(2, offset)
            return offset, left_below, left_above

        offset, left_below, left_above = lax.cond(own >= 512, with_chunks, gather_beside, own)
        offset = gather_others(offset, (left_own, left_below, left_above))
        done = jnp.where(own >= 512, 1, 0)
        prepare(held0, done * 2, offset)

        def two_chunks(at, carry):
            stream(held0, sums)
            prepare(held1, at * 2 + 1, offset)
            stream(held1, sums)
            prepare(held0, at * 2 + 2, offset)
            return carry

        chunks = lax.shift_right_logical(offset + 255, 8)
        lax.fori_loop(done, lax.shift_right_logical(chunks, 1), two_chunks, 0)

        @pl.when(lax.bitwise_and(chunks, 1) == 1)
        def _():
            stream(held0, sums)

        @pl.when(lax.bitwise_and(chunks, 1) == 0)
        def _():
            for unit in range(2):
                pltpu.matmul_acc_lhs(sums[unit][0], jnp.zeros((ROWS, 256), BF16), load_staged_rhs=0)

        lines = flat.reshape(ROWS * PLANES * 6, 128)
        for plane in range(2 * PLANES):
            z, c = plane // 2, plane % 2
            sides = [pltpu.matmul_pop(sums[unit][plane]) for unit in range(2)]
            for y in range(3):
                lines[pl.ds(z * 6 + y * 2 + c, ROWS, stride=36), :] = sides[y // 2][:, (y % 2) * 128 : (y % 2) * 128 + 128]

    pl.run_scoped(run, *[pltpu.ACC(unit)((ROWS, 256), F32) for unit in range(2) for _ in range(12)])
    copies = [pltpu.make_async_copy(flat.at[:, y], out_ref.at[:, :, pl.ds(y * 128, 128)], out_sem.at[y]) for y in range(3)]
    for copy in copies:
        copy.start()
    for copy in copies:
        copy.wait()


def grid_block(everything, group=None):
    vmem = pl.BlockSpec(memory_space=pltpu.VMEM)
    if group is None:
        operands, specs = [everything], [vmem]

        def kernel(all_ref, *refs):
            grid_kernel(lambda: lax.axis_index("grp"), all_ref, *refs)
    else:
        operands, specs = [group, everything], [pl.BlockSpec(memory_space=pltpu.SMEM), vmem]

        def kernel(group_ref, all_ref, *refs):
            grid_kernel(lambda: group_ref[0], all_ref, *refs)

    return pl.pallas_call(
        kernel,
        out_shape=jax.ShapeDtypeStruct((ROWS * PLANES, 2, NY), F32),
        in_specs=specs,
        out_specs=pl.BlockSpec(memory_space=pl.ANY),
        scratch_shapes=[
            pltpu.VMEM((SOURCES, 128), I32),
            pltpu.SMEM((SOURCES, 128), I32),
            pltpu.VMEM((388, 8, 128), F32),
            pltpu.VMEM((2, 4, 8, 128), F32),
            pltpu.VMEM((2, 4, 8, 128), F32),
            pltpu.VMEM((ROWS * PLANES, 3, 2, 128), F32),
            pltpu.SemaphoreType.DMA,
            pltpu.SemaphoreType.DMA((3,)),
        ],
        compiler_params=pltpu.CompilerParams(vmem_limit_bytes=16 * 2**20),
        name="grid_block",
    )(*operands)


def shards(sample_xy, sample_dz, sample_values, block_tile, block_count):
    operands = [block_tile, block_count, sample_xy.reshape(8, 2, 256), sample_dz.reshape(8, 256), sample_values.reshape(8, 2, 256)]
    everything = exchange(*[pltpu.with_memory_space_constraint(operand, pltpu.HBM) for operand in operands])
    block = grid_block(everything.reshape(SOURCES * SEND_ROWS, 128))
    return block.reshape(ROWS, PLANES, 2, NY)


def solution(mesh):
    return jax.shard_map(
        shards,
        mesh=mesh,
        in_specs=(
            P("grp", "slab", None, None, None),
            P("grp", "slab", None, None),
            P("grp", "slab", None, None, None),
            P("grp", "slab", None),
            P("grp", "slab", None),
        ),
        out_specs=P("grp", "slab", None, None),
        check_vma=False,
    )
```

```python
import math

import jax
import jax.numpy as jnp
from jax import lax
from jax.experimental import pallas as pl
from jax.experimental.pallas import tpu as pltpu
from jax.sharding import PartitionSpec as P

NX = 384
NY = 384
PLANES = 6
BLOCKS = 8
GROUPS = 8
ROWS = 48
FIELDS = 5
HALF_ROWS = FIELDS * BLOCKS
TABLE = 2 * HALF_ROWS
SEND_ROWS = TABLE + BLOCKS
SOURCES = 3 * GROUPS
LOW, COUNT, LEFT, WRAP, WRAP_LEFT, ANY_LEFT, HIGH = 0, 8, 32, 56, 80, 104, 112
PIECES = [(0, HALF_ROWS), (HALF_ROWS, SEND_ROWS - HALF_ROWS)]
ORDER = (1, 2, 0)
MESH = pl.DeviceIdType.MESH
BETA = math.pi * math.sqrt(19.45)
F32 = jnp.float32
BF16 = jnp.bfloat16
I32 = jnp.int32


def kaiser_coefficients():
    half_sq = (0.5 * BETA) ** 2
    terms = []
    term = 1.0
    for order in range(1, 32):
        term = term * half_sq / (order * order)
        terms.append(term)
    top = sum(terms)
    return [value / top for value in terms]


COEFF = kaiser_coefficients()


def kaiser(distance):
    third = distance * (1.0 / 3.0)
    inside = jnp.maximum(1.0 - third * third, 0.0)
    square = inside * inside
    fourth = square * square
    chains = []
    for first in range(4):
        picked = COEFF[first::4]
        total = jnp.full_like(inside, picked[-1])
        for value in picked[-2::-1]:
            total = total * fourth + value
        chains.append(total)
    low = chains[0] + chains[1] * inside
    high = chains[2] + chains[3] * inside
    return (low + high * square) * inside


def sort_blocks(tile_ref, count_ref, xy_ref, dz_ref, val_ref, out_ref, fields):
    lanes = lax.broadcasted_iota(I32, (BLOCKS, 256), 1)
    subs = lax.broadcasted_iota(I32, (BLOCKS, 256), 0)
    counts = jnp.zeros((BLOCKS, 256), I32)
    tiles = jnp.zeros((BLOCKS, 256), I32)
    for b in range(BLOCKS):
        counts = jnp.where(subs == b, count_ref[0, 0, b], counts)
        tiles = jnp.where(subs == b, tile_ref[0, 0, b], tiles)
    along_x = xy_ref[:, 0, :]
    cell = jnp.floor(along_x)
    shifted = cell + 3.0
    shifted = jnp.where(shifted >= NX, shifted - NX, shifted)
    shifted = jnp.where(lanes < counts, shifted, 400.0)
    fields[0:8] = along_x
    fields[8:16] = xy_ref[:, 1, :]
    fields[16:24] = dz_ref[...] + tiles.astype(F32)
    fields[24:32] = val_ref[:, 0, :]
    fields[32:40] = val_ref[:, 1, :]

    def below(bound):
        return jnp.sum(jnp.where(shifted < bound, 1.0, 0.0), axis=1, keepdims=True)

    column = lanes[:, 0:128]
    tile_f = tiles[:, 0:128].astype(F32)
    kinds = [jnp.ones((BLOCKS, 128), F32), jnp.where(tile_f > 2.5, 1.0, 0.0), jnp.where(tile_f < 1.5, 1.0, 0.0)]
    table = jnp.zeros((BLOCKS, 128), F32)
    for group in range(GROUPS):
        start = below(float(ROWS * group))
        count = below(float(ROWS * group + ROWS + 5)) - start
        first = jnp.minimum(count, 128.0)
        start = jnp.minimum(start, 255.0)
        high = jnp.where(start > 127.5, 1.0, 0.0)
        table = jnp.where(column == LOW + group, start - 128.0 * high, table)
        table = jnp.where(column == HIGH + group, high * HALF_ROWS, table)
        for kind in range(3):
            table = jnp.where(column == COUNT + 8 * kind + group, first * kinds[kind], table)
            table = jnp.where(column == LEFT + 8 * kind + group, (count - first) * kinds[kind], table)
    count = below(5.0)
    first = jnp.minimum(count, 128.0)
    for kind in range(3):
        table = jnp.where(column == WRAP + kind, first * kinds[kind], table)
        table = jnp.where(column == WRAP + 3 + kind, (count - first) * kinds[kind], table)
    table = table.T
    pieces = [table[at : at + 8] for at in range(0, WRAP, 8)]
    pieces += [jnp.broadcast_to(table[WRAP + at : WRAP + at + 1], (8, 8)) for at in range(6)]
    left = pieces[4] + pieces[10]
    pieces.append(jnp.broadcast_to(jnp.sum(left, axis=1, keepdims=True), (8, 8)))
    pieces.append(table[HIGH : HIGH + 8])
    out_ref[TABLE : TABLE + BLOCKS, :] = jnp.concatenate(pieces + [jnp.zeros((8, 128 - 8 * len(pieces)), F32)], axis=1)
    key = shifted * 256.0 + lanes.astype(F32)
    key_t = key.T
    place = lax.broadcasted_iota(I32, (256, 256), 0).astype(F32)
    for b in range(BLOCKS):
        before = key_t[:, b : b + 1] < key[b : b + 1, :]
        rank = jnp.sum(jnp.where(before, 1.0, 0.0), axis=0, keepdims=True)
        pick = jnp.where(place == rank, 1.0, 0.0).astype(BF16)
        rows = jnp.concatenate([fields[f * 8 + b : f * 8 + b + 1, :] for f in range(5)] + [jnp.zeros((3, 256), F32)], axis=0)
        top = rows.astype(BF16)
        rest = rows - top.astype(F32)
        mid = rest.astype(BF16)
        low = (rest - mid.astype(F32)).astype(BF16)
        parts = jnp.concatenate([top.astype(F32), mid.astype(F32), low.astype(F32)], axis=0).astype(BF16)
        moved = lax.dot_general(parts, pick, (((1,), (1,)), ((), ())), preferred_element_type=F32)
        ordered = (moved[0:8] + moved[8:16]) + moved[16:24]
        for f in range(FIELDS):
            for half in range(2):
                row = half * HALF_ROWS + f * 8 + b
                out_ref[row : row + 1, :] = ordered[f : f + 1, half * 128 : half * 128 + 128]


def exchange_kernel(
    tile_in, count_in, xy_in, dz_in, val_in, out_ref, tile_ref, count_ref, xy_ref, dz_ref, val_ref, fields, own_ref, in_sem, send_sem, recv_sem
):
    loads = [
        pltpu.make_async_copy(source, target, in_sem.at[at])
        for at, (source, target) in enumerate(
            [(xy_in, xy_ref), (tile_in, tile_ref), (count_in, count_ref), (dz_in, dz_ref), (val_in, val_ref)]
        )
    ]
    for load in loads:
        load.start()
    grp = lax.axis_index("grp")
    slab = lax.axis_index("slab")
    far = lax.rem(grp + 4, 8)
    half = (grp // 4) * 4
    spot = grp - half
    peers = [half + lax.rem(spot + step, 4) for step in (2, 1, 3)]
    far_half = 4 - half
    core = lax.rem(slab, 2)
    outer = lax.rem(slab + 31 - 30 * core, 32)
    inner = lax.rem(slab + 1 + 30 * core, 32)
    beside = [((grp, outer), 2 - core), ((grp, inner), 1 + core)]
    around = [(far, slab)] + [(peer, slab) for peer in peers] + [(grp, outer), (grp, inner)]

    barrier = pltpu.get_barrier_semaphore()
    for device in around:
        pl.semaphore_signal(barrier, inc=1, device_id=device, device_id_type=MESH)
    for load in loads:
        load.wait()
    sort_blocks(tile_ref, count_ref, xy_ref, dz_ref, val_ref, own_ref, fields)
    pl.semaphore_wait(barrier, len(around))

    sends = []

    def rows_of(ref, rows):
        return ref if rows is None else ref.at[pl.ds(rows[0], rows[1])]

    def send(source, kind, owner, item, device, rows=None):
        copy = pltpu.make_async_remote_copy(
            src_ref=rows_of(source, rows),
            dst_ref=rows_of(out_ref.at[kind, owner], rows),
            send_sem=send_sem.at[len(sends)],
            recv_sem=recv_sem.at[kind, item],
            device_id=device,
            device_id_type=MESH,
        )
        copy.start()
        sends.append(copy)

    def arrive(kind, owner, item, rows=None):
        pltpu.make_async_remote_copy(
            src_ref=rows_of(own_ref, rows),
            dst_ref=rows_of(out_ref.at[kind, owner], rows),
            send_sem=send_sem.at[0],
            recv_sem=recv_sem.at[kind, item],
            device_id=(grp, slab),
            device_id_type=MESH,
        ).wait_recv()

    pieces = PIECES
    count = len(pieces)
    for at, rows in enumerate(pieces):
        send(own_ref, 0, grp, 4 + at, (far, slab), rows)
    for at, peer in enumerate(peers):
        send(own_ref, 0, grp, 1 + at, (peer, slab))
    for device, kind in beside:
        send(own_ref, kind, grp, 0, device)
    out_ref[0, grp] = own_ref[...]
    back = [half + lax.rem(spot + step, 4) for step in (2, 3, 1)]
    for at in ORDER:
        arrive(0, back[at], 1 + at)
        for device, kind in beside:
            send(out_ref.at[0, back[at]], kind, back[at], 1 + at, device)
    for piece, rows in enumerate(pieces):
        arrive(0, far, 4 + piece, rows)
        for at, peer in enumerate(peers):
            send(out_ref.at[0, far], 0, far, 4 + count + count * at + piece, (peer, slab), rows)
        for device, kind in beside:
            send(out_ref.at[0, far], kind, far, 4 + piece, device, rows)
    for piece, rows in enumerate(pieces):
        for at in ORDER:
            owner = back[at] - half + far_half
            arrive(0, owner, 4 + count + count * at + piece, rows)
            for device, kind in beside:
                send(out_ref.at[0, owner], kind, owner, 4 + count + count * at + piece, device, rows)
    for kind in (1, 2):
        arrive(kind, grp, 0)
        for at in range(3):
            arrive(kind, back[at], 1 + at)
        for piece, rows in enumerate(pieces):
            arrive(kind, far, 4 + piece, rows)
            for at in range(3):
                arrive(kind, back[at] - half + far_half, 4 + count + count * at + piece, rows)
    for copy in sends:
        copy.wait_send()


def exchange(tile, count, xy, dz, val):
    vmem = pl.BlockSpec(memory_space=pltpu.VMEM)
    hbm = pl.BlockSpec(memory_space=pltpu.HBM)
    return pl.pallas_call(
        exchange_kernel,
        out_shape=jax.ShapeDtypeStruct((3, GROUPS, SEND_ROWS, 128), F32),
        in_specs=[hbm] * 5,
        out_specs=vmem,
        scratch_shapes=[
            pltpu.SMEM((1, 1, 8), I32),
            pltpu.SMEM((1, 1, 8), I32),
            pltpu.VMEM((BLOCKS, 2, 256), F32),
            pltpu.VMEM((BLOCKS, 256), F32),
            pltpu.VMEM((BLOCKS, 2, 256), F32),
            pltpu.VMEM((HALF_ROWS, 256), F32),
            pltpu.VMEM((SEND_ROWS, 128), F32),
            pltpu.SemaphoreType.DMA((5,)),
            pltpu.SemaphoreType.DMA((11 + 12 * len(PIECES),)),
            pltpu.SemaphoreType.DMA((3, 4 + 4 * len(PIECES))),
        ],
        compiler_params=pltpu.CompilerParams(collective_id=0, has_side_effects=True, vmem_limit_bytes=8 * 2**20),
        name="exchange",
    )(tile, count, xy, dz, val)


def grid_kernel(read_group, all_ref, out_ref, table_v, table, packed, held0, held1, flat, sem, out_sem):
    group = read_group()
    for source in range(SOURCES):
        table_v[source : source + 1, :] = all_ref[pl.ds(source * SEND_ROWS + TABLE + group, 1), :].astype(I32)
    tables = [pltpu.make_async_copy(table_v.at[pl.ds(at, 8)], table.at[pl.ds(at, 8)], sem.at[at // 8]) for at in (0, 8, 16)]
    for copy in tables:
        copy.start()
    lanes = lax.broadcasted_iota(I32, (8, 128), 1)
    lanes_f = lanes[:FIELDS]
    subs = lax.broadcasted_iota(I32, (8, 128), 0)

    def append(kind, source, b, low, rows, count, offset):
        first = source * SEND_ROWS + b
        values = all_ref[pl.ds(first + rows, FIELDS, stride=8), :]
        after = all_ref[pl.ds(first + HALF_ROWS, FIELDS, stride=8), :]
        values = jnp.where(lanes_f >= low, values, after)
        if kind > 0:
            values = values + jnp.where(subs[:FIELDS] == 2, (0.0, -6.0, 6.0)[kind], 0.0)
        at = lax.bitwise_and(offset, 127)
        rolled = pltpu.roll(values, lax.bitwise_and(at - low, 127), 1)
        slot = lax.shift_right_logical(offset, 7)
        pltpu.store(packed.at[slot, 0:FIELDS], rolled, mask=lanes_f >= at)
        packed[slot + 1, 0:FIELDS] = rolled
        return offset + count

    def span(wrap, source, b):
        return (jnp.int32(0), jnp.int32(0)) if wrap else (table[source, LOW + b], table[source, HIGH + b])

    def gather(kind, wrap):
        def body(at, carry):
            offset, more = carry
            source = kind * GROUPS + at
            for b in range(BLOCKS):
                low, rows = span(wrap, source, b)
                offset = append(kind, source, b, low, rows, table[source, (WRAP if wrap else COUNT) + 8 * kind + b], offset)
            return offset, more + table[source, ANY_LEFT]

        return body

    def gather_rest(kind, wrap):
        def body(at, offset):
            source = kind * GROUPS + lax.shift_right_logical(at, 3)
            b = lax.bitwise_and(at, 7)
            low = span(wrap, source, b)[0]
            left = table[source, (WRAP_LEFT if wrap else LEFT) + 8 * kind + b]
            return lax.cond(left > 0, lambda o: append(kind, source, b, low, HALF_ROWS, left, o), lambda o: o, offset)

        return body

    def gather_kind(kind, offset):
        more = jnp.int32(0)
        for at in range(GROUPS):
            offset, more = gather(kind, False)(at, (offset, more))
        return offset, more

    def gather_others(offset, left):
        for kind in range(3):
            offset = lax.fori_loop(0, jnp.where(left[kind] > 0, 64, 0), gather_rest(kind, False), offset)
        for kind in range(3):
            steps = jnp.where(group == GROUPS - 1, GROUPS, 0)
            offset, more = lax.fori_loop(0, steps, gather(kind, True), (offset, jnp.int32(0)))
            offset = lax.fori_loop(0, jnp.where(more > 0, 64, 0), gather_rest(kind, True), offset)
        return offset

    subs_f = subs.astype(F32)
    first_row = (group * ROWS).astype(F32)

    def place(taps, base):
        away = subs_f - base
        part = -jnp.floor(away * 0.125)
        index = (away + 8.0 * part).astype(I32)
        turned = jnp.take_along_axis(taps, index, axis=0, mode="promise_in_bounds")
        part = jnp.where(part < 0.0, part + 48.0, part)
        part = jnp.where(part >= 48.0, part - 48.0, part)
        return turned, part

    def pair(part):
        return jnp.concatenate([part, part - 1.0], axis=0).astype(BF16)

    def twice(value):
        return jnp.concatenate([value, value], axis=0).astype(BF16)

    zero = jnp.zeros((16, 128), BF16)

    def prepare(held, at, offset):
        sides = []
        for half in range(2):
            values = packed[at * 2 + half]
            values = jnp.where(lanes + (at * 256 + half * 128) < offset, values, 0.0)
            along_x, along_y, along_z = [jnp.broadcast_to(values[f : f + 1], (8, 128)) for f in range(3)]
            cell_x = jnp.floor(along_x)
            cell_y = jnp.floor(along_y)
            taps_x = kaiser(subs_f - 2.0 - (along_x - cell_x)).astype(BF16).astype(F32)
            taps_y = kaiser(subs_f - 2.0 - (along_y - cell_y))
            taps_z = kaiser(subs_f - along_z)
            turned_x, part_x = place(taps_x, cell_x - 2.0 - first_row)
            turned_y, part_y = place(taps_y, cell_y - 2.0)
            held[half, 0] = turned_x
            held[half, 1] = part_x
            for c in range(2):
                held[half, 2 + c] = taps_z * jnp.broadcast_to(values[3 + c : 4 + c], (8, 128))
            turned_y, part_y = twice(turned_y), pair(part_y)
            sides.append([jnp.where(part_y == group_y, turned_y, zero) for group_y in range(0, NY // 8, 2)] + [zero] * 8)
        for unit in range(2):
            tiles = [jnp.concatenate([side[unit * 16 + at] for side in sides], axis=1) for at in range(16)]
            pltpu.matmul_push_rhs(jnp.concatenate(tiles, axis=0), staging_register=0, mxu_index=unit, transpose=True)

    def stream(held, sums):
        here = []
        for half in range(2):
            part_x = pair(held[half, 1])
            here.append([part_x == group_x for group_x in range(0, ROWS // 8, 2)])
        for plane in range(2 * PLANES):
            z, c = plane // 2, plane % 2
            sides = []
            for half in range(2):
                scaled = twice(held[half, 0] * jnp.broadcast_to(held[half, 2 + c, z : z + 1], (8, 128)))
                sides.append([jnp.where(mask, scaled, zero) for mask in here[half]])
            rows = jnp.concatenate([jnp.concatenate([side[at] for side in sides], axis=1) for at in range(3)], axis=0)
            for unit in range(2):
                pltpu.matmul_acc_lhs(sums[unit][plane], rows, load_staged_rhs=0 if plane == 0 else None)

    def run(*accumulators):
        sums = (accumulators[:12], accumulators[12:])
        tables[0].wait()
        own, left_own = gather_kind(0, jnp.int32(0))
        tables[1].wait()
        tables[2].wait()

        def gather_beside(offset):
            offset, left_below = gather_kind(1, offset)
            offset, left_above = gather_kind(2, offset)
            return offset, left_below, left_above

        def with_chunks(offset):
            prepare(held0, 0, offset)
            prepare_next = offset
            stream(held0, sums)
            offset, left_below = gather_kind(1, offset)
            prepare(held1, 1, prepare_next)
            stream(held1, sums)
            offset, left_above = gather_kind(2, offset)
            return offset, left_below, left_above

        offset, left_below, left_above = lax.cond(own >= 512, with_chunks, gather_beside, own)
        offset = gather_others(offset, (left_own, left_below, left_above))
        done = jnp.where(own >= 512, 1, 0)
        prepare(held0, done * 2, offset)

        def two_chunks(at, carry):
            stream(held0, sums)
            prepare(held1, at * 2 + 1, offset)
            stream(held1, sums)
            prepare(held0, at * 2 + 2, offset)
            return carry

        chunks = lax.shift_right_logical(offset + 255, 8)
        lax.fori_loop(done, lax.shift_right_logical(chunks, 1), two_chunks, 0)

        @pl.when(lax.bitwise_and(chunks, 1) == 1)
        def _():
            stream(held0, sums)

        @pl.when(lax.bitwise_and(chunks, 1) == 0)
        def _():
            for unit in range(2):
                pltpu.matmul_acc_lhs(sums[unit][0], jnp.zeros((ROWS, 256), BF16), load_staged_rhs=0)

        lines = flat.reshape(ROWS * PLANES * 6, 128)
        for plane in range(2 * PLANES):
            z, c = plane // 2, plane % 2
            sides = [pltpu.matmul_pop(sums[unit][plane]) for unit in range(2)]
            for y in range(3):
                lines[pl.ds(z * 6 + y * 2 + c, ROWS, stride=36), :] = sides[y // 2][:, (y % 2) * 128 : (y % 2) * 128 + 128]

    pl.run_scoped(run, *[pltpu.ACC(unit)((ROWS, 256), F32) for unit in range(2) for _ in range(12)])
    copies = [pltpu.make_async_copy(flat.at[:, y], out_ref.at[:, :, pl.ds(y * 128, 128)], out_sem.at[y]) for y in range(3)]
    for copy in copies:
        copy.start()
    for copy in copies:
        copy.wait()


def grid_block(everything, group=None):
    vmem = pl.BlockSpec(memory_space=pltpu.VMEM)
    if group is None:
        operands, specs = [everything], [vmem]

        def kernel(all_ref, *refs):
            grid_kernel(lambda: lax.axis_index("grp"), all_ref, *refs)
    else:
        operands, specs = [group, everything], [pl.BlockSpec(memory_space=pltpu.SMEM), vmem]

        def kernel(group_ref, all_ref, *refs):
            grid_kernel(lambda: group_ref[0], all_ref, *refs)

    return pl.pallas_call(
        kernel,
        out_shape=jax.ShapeDtypeStruct((ROWS * PLANES, 2, NY), F32),
        in_specs=specs,
        out_specs=pl.BlockSpec(memory_space=pl.ANY),
        scratch_shapes=[
            pltpu.VMEM((SOURCES, 128), I32),
            pltpu.SMEM((SOURCES, 128), I32),
            pltpu.VMEM((388, 8, 128), F32),
            pltpu.VMEM((2, 4, 8, 128), F32),
            pltpu.VMEM((2, 4, 8, 128), F32),
            pltpu.VMEM((ROWS * PLANES, 3, 2, 128), F32),
            pltpu.SemaphoreType.DMA((3,)),
            pltpu.SemaphoreType.DMA((3,)),
        ],
        compiler_params=pltpu.CompilerParams(vmem_limit_bytes=16 * 2**20),
        name="grid_block",
    )(*operands)


def shards(sample_xy, sample_dz, sample_values, block_tile, block_count):
    operands = [block_tile, block_count, sample_xy.reshape(8, 2, 256), sample_dz.reshape(8, 256), sample_values.reshape(8, 2, 256)]
    everything = exchange(*[pltpu.with_memory_space_constraint(operand, pltpu.HBM) for operand in operands])
    block = grid_block(everything.reshape(SOURCES * SEND_ROWS, 128))
    return block.reshape(ROWS, PLANES, 2, NY)


def solution(mesh):
    return jax.shard_map(
        shards,
        mesh=mesh,
        in_specs=(
            P("grp", "slab", None, None, None),
            P("grp", "slab", None, None),
            P("grp", "slab", None, None, None),
            P("grp", "slab", None),
            P("grp", "slab", None),
        ),
        out_specs=P("grp", "slab", None, None),
        check_vma=False,
    )
```
